128 devices in a mesh: rep: 1, ep: 2 (over core), fsdp: 64 (over z, y, x).
Axes of the slice: x: 4, y: 4, z: 4, core: 2. Of those that a mesh axis runs over, the one named last changes fastest.
Arguments:
- x_in: bfloat16 [65536, 1024], P(('rep', 'ep', 'fsdp'))
- norm_w: float32 [2, 1024], replicated
- router_w: bfloat16 [2, 1024, 32], replicated
- gate_w: bfloat16 [2, 32, 1024, 512], P(None, 'ep', None, 'fsdp')
- up_w: bfloat16 [2, 32, 1024, 512], P(None, 'ep', None, 'fsdp')
- down_w: bfloat16 [2, 32, 512, 1024], P(None, 'ep', 'fsdp')
- routes: int32 [2, 65536, 8], P(None, ('rep', 'ep', 'fsdp'))
Outputs:
- output: bfloat16 [65536, 1024], P(('rep', 'ep', 'fsdp'))
All inputs are finite; a program needn't handle non-finite values.
Results may differ from the reference program's by a relative error of at most 0.00733116.
Values are sent between devices in bfloat16 or wider.
A program may use at most 1 GiB of HBM per device.

```python
import jax
import jax.numpy as jnp
from jax import lax
import numpy as np

EXPERTS = 32
TOP = 8
D_MODEL = 1024
FF_DIM = 512
TOK_DEV = 512
DEV_PART = 128
LAYERS = 2

NORM_EPS = 1e-5
CAPACITY = 8 * ((2 * TOK_DEV * TOP + 8 * EXPERTS - 1) // (8 * EXPERTS))
TOKENS = TOK_DEV * DEV_PART
ROW_CAP = DEV_PART * CAPACITY


def count_pattern(n_pairs, n_experts, capacity):
    counts = [1 + ((capacity - 1) * (n_experts - 1 - position)) // (n_experts - 1) for position in range(n_experts)]
    cursor = 1
    while sum(counts) < n_pairs:
        if counts[cursor] < capacity:
            counts[cursor] += 1
        cursor = cursor % (n_experts - 1) + 1
    while sum(counts) > n_pairs:
        if counts[cursor] > 1:
            counts[cursor] -= 1
        cursor = cursor % (n_experts - 1) + 1
    return counts


def draw_routes(route_key):
    counts = count_pattern(TOK_DEV * TOP, EXPERTS, CAPACITY)
    pattern = np.repeat(np.arange(EXPERTS), counts).astype(np.int32)

    def one_block(block_key):
        key_label, key_order = jax.random.split(block_key)
        relabel = jax.random.permutation(key_label, EXPERTS)
        expert_ids = relabel[pattern].reshape(TOP, TOK_DEV).T
        token_order = jax.random.permutation(key_order, TOK_DEV)
        return expert_ids[token_order]

    block_keys = jax.random.split(route_key, LAYERS * DEV_PART)
    all_blocks = jax.vmap(one_block)(block_keys)
    return all_blocks.reshape(LAYERS, TOKENS, TOP).astype(jnp.int32)


def setup_inputs(seed: int = 0, part: int = 0) -> dict:
    weight_keys = jax.random.split(jax.random.key(seed), 5)
    part_keys = jax.random.split(jax.random.fold_in(jax.random.key(seed + 1), part), 2)
    x_in = jax.random.normal(part_keys[0], (TOKENS, D_MODEL), jnp.float32).astype(jnp.bfloat16)
    norm_w = 1.0 + 0.25 * jax.random.normal(weight_keys[0], (LAYERS, D_MODEL), jnp.float32)
    router_w = (jax.random.normal(weight_keys[1], (LAYERS, D_MODEL, EXPERTS), jnp.float32) * D_MODEL ** -0.5).astype(jnp.bfloat16)
    gate_w = (jax.random.normal(weight_keys[2], (LAYERS, EXPERTS, D_MODEL, FF_DIM), jnp.float32) * D_MODEL ** -0.5).astype(jnp.bfloat16)
    up_w = (jax.random.normal(weight_keys[3], (LAYERS, EXPERTS, D_MODEL, FF_DIM), jnp.float32) * D_MODEL ** -0.5).astype(jnp.bfloat16)
    down_w = (jax.random.normal(weight_keys[4], (LAYERS, EXPERTS, FF_DIM, D_MODEL), jnp.float32) * (1.5 * (TOP / FF_DIM) ** 0.5)).astype(jnp.bfloat16)
    routes = draw_routes(part_keys[1])
    return {"x_in": x_in, "norm_w": norm_w, "router_w": router_w, "gate_w": gate_w, "up_w": up_w, "down_w": down_w, "routes": routes}


def rms_norm(stream, norm_row):
    widened = stream.astype(jnp.float32)
    inv_rms = lax.rsqrt(jnp.mean(widened * widened, axis=-1, keepdims=True) + NORM_EPS)
    return (widened * inv_rms * norm_row).astype(jnp.bfloat16)


def moe_layer(stream, layer_params):
    norm_row, router_l, gate_l, up_l, down_l, routes_l = layer_params
    hidden = rms_norm(stream, norm_row)
    logits = jnp.dot(hidden, router_l, preferred_element_type=jnp.float32)
    gate_probs = jax.nn.softmax(jnp.take_along_axis(logits, routes_l, axis=1), axis=-1)

    def expert_step(mixed_sum, expert_params):
        expert_id, gate_e, up_e, down_e = expert_params
        is_chosen = routes_l == expert_id
        token_gate = jnp.sum(jnp.where(is_chosen, gate_probs, 0.0), axis=1)
        token_rows = jnp.nonzero(jnp.any(is_chosen, axis=1), size=ROW_CAP, fill_value=0)[0]
        row_valid = jnp.arange(ROW_CAP) < jnp.sum(is_chosen)
        row_gate = jnp.where(row_valid, token_gate[token_rows], 0.0)
        picked = hidden[token_rows]
        pre_gate = jnp.dot(picked, gate_e, preferred_element_type=jnp.float32)
        pre_up = jnp.dot(picked, up_e, preferred_element_type=jnp.float32)
        inner_act = (jax.nn.silu(pre_gate) * pre_up).astype(jnp.bfloat16)
        expert_out = jnp.dot(inner_act, down_e, preferred_element_type=jnp.float32).astype(jnp.bfloat16)
        mixed_sum = mixed_sum.at[token_rows].add(row_gate[:, None] * expert_out.astype(jnp.float32))
        return mixed_sum, None

    start_sum = jnp.zeros(stream.shape, jnp.float32)
    mixed_sum, _ = lax.scan(expert_step, start_sum, (jnp.arange(EXPERTS), gate_l, up_l, down_l))
    return (stream.astype(jnp.float32) + mixed_sum).astype(jnp.bfloat16), None


def reference(x_in, norm_w, router_w, gate_w, up_w, down_w, routes):
    final_stream, _ = lax.scan(moe_layer, x_in, (norm_w, router_w, gate_w, up_w, down_w, routes))
    return final_stream
```

```python
import functools

import jax
import jax.numpy as jnp
from jax import lax
from jax.experimental import pallas as pl
from jax.experimental.pallas import tpu as pltpu
from jax.sharding import Mesh, PartitionSpec as P

NORM_EPS = 1e-5
MESH_ID = pl.DeviceIdType.MESH

O_A, O_B, R_B, L_A, R_A, L_B, F_A, F_B = range(8)
UNITS = 8


def rms_norm(stream, norm_row):
    widened = stream.astype(jnp.float32)
    inv_rms = lax.rsqrt(jnp.mean(widened * widened, axis=-1, keepdims=True) + NORM_EPS)
    return (widened * inv_rms * norm_row).astype(jnp.bfloat16)


def dense_gates(hidden, router_l, routes_l):
    experts = router_l.shape[1]
    logits = jnp.dot(hidden, router_l, preferred_element_type=jnp.float32)
    ids = jnp.arange(experts, dtype=routes_l.dtype)
    chosen = jnp.any(routes_l[:, :, None] == ids[None, None, :], axis=1)
    top = jnp.max(jnp.where(chosen, logits, -jnp.inf), axis=-1, keepdims=True)
    weight = jnp.where(chosen, jnp.exp(jnp.where(chosen, logits - top, 0.0)), 0.0)
    gates = weight / jnp.sum(weight, axis=-1, keepdims=True)
    return jnp.where(chosen, gates, -1.0).T


def layer_kernel(h_ref, g_ref, w_ref, x_ref, out_ref, h_all, g_all, w_v, acc, pair_in, ring_in,
                 own_sem, w_sem, ag_send, ag_recv, agp_send, agp_recv, pair_send, pair_recv, ring_send, ring_recv):
    half, d_model = h_all.shape[1] // 2, h_all.shape[2]
    n_exp = w_v.shape[0]
    ep, x = lax.axis_index("ep"), lax.axis_index("x")
    n_x = 4
    right = {"x": lax.rem(x + 1, n_x)}
    left = {"x": lax.rem(x + n_x - 1, n_x)}
    partner = {"ep": 1 - ep}
    group = ep * n_x + x

    barrier = pltpu.get_barrier_semaphore()
    for peer in (right, left, partner):
        pl.semaphore_signal(barrier, inc=1, device_id=peer, device_id_type=MESH_ID)

    own = []
    for unit in (O_A, O_B):
        rows = pl.ds((unit - O_A) * half, half)
        own.append(pltpu.make_async_copy(h_ref.at[rows], h_all.at[unit, pl.ds(0, half)], own_sem.at[2 * unit]))
        own.append(pltpu.make_async_copy(g_ref.at[:, rows], g_all.at[unit, 0], own_sem.at[2 * unit + 1]))
    for copy in own:
        copy.start()
    loads = [pltpu.make_async_copy(w_ref.at[:, e], w_v.at[e], w_sem.at[e]) for e in range(n_exp)]
    for copy in loads:
        copy.start()
    for copy in own:
        copy.wait()
    pl.semaphore_wait(barrier, 3)

    def gather_copy(idx, unit, dst, peer):
        return (
            pltpu.make_async_remote_copy(
                h_all.at[unit, pl.ds(0, half)], h_all.at[dst, pl.ds(0, half)],
                ag_send.at[2 * idx], ag_recv.at[2 * idx], device_id=peer, device_id_type=MESH_ID),
            pltpu.make_async_remote_copy(
                g_all.at[unit, 0], g_all.at[dst, 0],
                ag_send.at[2 * idx + 1], ag_recv.at[2 * idx + 1], device_id=peer, device_id_type=MESH_ID),
        )

    def pair_copy(unit):
        return (
            pltpu.make_async_remote_copy(
                h_all.at[unit, pl.ds(0, half)], h_all.at[unit, pl.ds(half, half)],
                agp_send.at[2 * unit], agp_recv.at[2 * unit], device_id=partner, device_id_type=MESH_ID),
            pltpu.make_async_remote_copy(
                g_all.at[unit, 0], g_all.at[unit, 1],
                agp_send.at[2 * unit + 1], agp_recv.at[2 * unit + 1], device_id=partner, device_id_type=MESH_ID),
        )

    moves = {
        L_A: (0, O_A, right), R_B: (1, O_B, left),
        L_B: (2, O_B, right), R_A: (3, O_A, left),
        F_A: (4, L_A, right), F_B: (5, R_B, left),
    }

    def ring_gather(dst):
        idx, src, peer = moves[dst]
        return gather_copy(idx, src, dst, peer)

    def start(copies):
        for copy in copies:
            copy.start()

    def wait_recv(copies):
        for copy in copies:
            copy.wait_recv()

    def wait_send(copies):
        for copy in copies:
            copy.wait_send()

    def reduce_pair(unit):
        return pltpu.make_async_remote_copy(
            acc.at[unit, pl.ds(half, half)], pair_in.at[unit],
            pair_send.at[unit], pair_recv.at[unit], device_id=partner, device_id_type=MESH_ID)

    sums = {R_B: (0, right), F_A: (1, right), R_A: (2, right), L_A: (3, left), F_B: (4, left), L_B: (5, left)}

    def reduce_ring(unit):
        slot, peer = sums[unit]
        return pltpu.make_async_remote_copy(
            acc.at[unit, pl.ds(0, half)], ring_in.at[slot],
            ring_send.at[slot], ring_recv.at[slot], device_id=peer, device_id_type=MESH_ID)

    def add_pair(unit):
        reduce_pair(unit).wait_recv()
        acc[unit, 0:half, :] += pair_in[unit]

    start(ring_gather(L_A))
    start(ring_gather(R_B))
    for unit in (O_A, O_B):
        start(pair_copy(unit))
    start(ring_gather(L_B))
    start(ring_gather(R_A))

    def at(step, t, action):
        @pl.when(step == t)
        def _():
            action()

    def arrive(*units):
        for unit in units:
            wait_recv(ring_gather(unit))
            if unit == L_A:
                start(ring_gather(F_A))
            if unit == R_B:
                start(ring_gather(F_B))
            start(pair_copy(unit))

    def step_fn(step, carry):
        unit, e = step // n_exp, step % n_exp
        for first_use, load in enumerate(loads):
            at(step, first_use, load.wait)
        at(step, 7, lambda: arrive(L_A, R_B))
        at(step, 14, lambda: arrive(L_B, R_A))
        at(step, 22, lambda: arrive(F_A, F_B))
        for k in range(UNITS):
            at(step, n_exp * k, lambda: wait_recv(pair_copy(k)))
            if k < UNITS - 1:
                at(step, n_exp * (k + 1), lambda: reduce_pair(k).start())
                if n_exp * (k + 1) + 2 < n_exp * UNITS:
                    at(step, n_exp * (k + 1) + 2, lambda: add_pair(k))
                    if k in (R_B, L_A, F_A):
                        at(step, n_exp * (k + 1) + 3, lambda: reduce_ring(k).start())

        tokens = h_all[unit]
        gate_w = w_v[e, :, 0].reshape(-1, d_model)
        up_w = w_v[e, :, 1].reshape(-1, d_model)
        down_w = w_v[e, :, 2].reshape(-1, d_model)
        d_ff = gate_w.shape[0]
        inner = []
        for f in range(0, d_ff, 256):
            nt = (((1,), (1,)), ((), ()))
            u = lax.dot_general(tokens, gate_w[f:f + 256], nt, preferred_element_type=jnp.float32)
            v = lax.dot_general(tokens, up_w[f:f + 256], nt, preferred_element_type=jnp.float32)
            inner.append((jax.nn.silu(u) * v).astype(jnp.bfloat16))
        inner = jnp.concatenate(inner, axis=1)
        row = group * n_exp + e
        gate_cols = []
        for s in range(2):
            gates = g_all[unit, s, pl.ds(row, 1), :]
            gate_cols.append(jnp.broadcast_to(gates, (128, half)).T)
        gate_b = jnp.concatenate(gate_cols, axis=0)
        gate_b = jnp.concatenate([gate_b, gate_b], axis=1)
        first = e == 0
        for c in range(0, d_model, 256):
            o = jnp.dot(inner, down_w[:, c:c + 256], preferred_element_type=jnp.float32)
            o = o.astype(jnp.bfloat16).astype(jnp.float32)
            part = jnp.where(gate_b >= 0.0, gate_b * o, 0.0)
            prev = jnp.where(first, 0.0, acc[unit, :, c:c + 256])
            acc[unit, :, c:c + 256] = prev + part
        return carry

    lax.fori_loop(0, UNITS * n_exp, step_fn, 0)

    last = UNITS - 1
    reduce_pair(last).start()
    for unit in (last,):
        add_pair(unit)
        reduce_ring(unit).start()
    reduce_ring(F_A).wait_recv()
    acc[R_A, 0:half, :] += ring_in[1]
    reduce_ring(R_A).start()
    reduce_ring(F_B).wait_recv()
    acc[L_B, 0:half, :] += ring_in[4]
    reduce_ring(L_B).start()

    reduce_ring(R_B).wait_recv()
    reduce_ring(L_A).wait_recv()
    acc[O_B, 0:half, :] += x_ref[half:, :].astype(jnp.float32) + ring_in[0]
    acc[O_A, 0:half, :] += x_ref[:half, :].astype(jnp.float32) + ring_in[3]
    reduce_ring(R_A).wait_recv()
    out_ref[0:half, :] = (acc[O_A, 0:half, :] + ring_in[2]).astype(out_ref.dtype)
    reduce_ring(L_B).wait_recv()
    out_ref[half:, :] = (acc[O_B, 0:half, :] + ring_in[5]).astype(out_ref.dtype)

    for unit in range(UNITS):
        wait_send(pair_copy(unit))
        reduce_pair(unit).wait_send()
        if unit in moves:
            wait_send(ring_gather(unit))
        if unit in sums:
            reduce_ring(unit).wait_send()


def moe_layer(idx, hidden, gates, weights, stream):
    tok_dev, d_model = hidden.shape
    half = tok_dev // 2
    n_exp = weights.shape[1]
    vmem = pl.BlockSpec(memory_space=pltpu.VMEM)
    hbm = pl.BlockSpec(memory_space=pl.ANY)
    dma = pltpu.SemaphoreType.DMA
    return pl.pallas_call(
        layer_kernel,
        name="moe_layer",
        out_shape=jax.ShapeDtypeStruct(stream.shape, stream.dtype),
        in_specs=[hbm, hbm, hbm, vmem],
        out_specs=vmem,
        scratch_shapes=[
            pltpu.VMEM((UNITS, tok_dev, d_model), jnp.bfloat16),
            pltpu.VMEM((UNITS, 2, gates.shape[0], half), jnp.float32),
            pltpu.VMEM((n_exp, weights.shape[0]) + weights.shape[2:], jnp.bfloat16),
            pltpu.VMEM((UNITS, tok_dev, d_model), jnp.float32),
            pltpu.VMEM((UNITS, half, d_model), jnp.float32),
            pltpu.VMEM((6, half, d_model), jnp.float32),
            dma((4,)), dma((n_exp,)),
            dma((12,)), dma((12,)), dma((16,)), dma((16,)), dma((8,)), dma((8,)), dma((6,)), dma((6,)),
        ],
        compiler_params=pltpu.CompilerParams(
            collective_id=0, has_side_effects=True, vmem_limit_bytes=67043328),
        cost_estimate=pl.CostEstimate(flops=52 * 10**9, bytes_accessed=16 * 2**20, transcendentals=0),
    )(hidden, gates, weights, stream)


def solution(mesh):
    n_x = 4
    n_y = min(4, mesh.shape["fsdp"] // n_x)
    devices = mesh.devices.reshape(mesh.shape["rep"], mesh.shape["ep"], -1, n_y, n_x)
    cells = Mesh(devices, ("rep", "ep", "z", "y", "x"))
    fsdp = ("z", "y", "x")
    token_spec = P(("rep", "ep") + fsdp, None)
    expert_in_spec = P(None, "ep", None, fsdp)
    expert_out_spec = P(None, "ep", fsdp, None)
    route_spec = P(None, ("rep", "ep") + fsdp, None)

    def device_step(x_in, norm_w, router_w, gate_w, up_w, down_w, routes):
        layers = routes.shape[0]
        n_local = gate_w.shape[1]
        n_exp = n_local // n_x
        f_dev = gate_w.shape[3]
        d_model = x_in.shape[1]

        stacked = jnp.stack([gate_w.transpose(0, 1, 3, 2), up_w.transpose(0, 1, 3, 2), down_w], axis=2)
        stacked = stacked.reshape(layers, n_x, n_exp, 3, f_dev, d_model)
        swapped = lax.all_to_all(stacked, "x", 1, 1, tiled=True)
        swapped = swapped.transpose(0, 2, 3, 1, 4, 5).reshape(layers, 1, n_exp, 3, n_x * f_dev, d_model)
        full = [lax.all_gather(swapped[l], ("z", "y"), axis=0, tiled=True) for l in range(layers)]

        stream = x_in
        for l in range(layers):
            hidden = rms_norm(stream, norm_w[l])
            gates = dense_gates(hidden, router_w[l], routes[l])
            stream = moe_layer(l, hidden, gates, full[l], stream)
        return stream

    return jax.shard_map(device_step, mesh=cells,
                         in_specs=(token_spec, P(), P(), expert_in_spec, expert_in_spec, expert_out_spec, route_spec),
                         out_specs=token_spec, check_vma=False)
```

```python
import functools

import jax
import jax.numpy as jnp
from jax import lax
from jax.experimental import pallas as pl
from jax.experimental.pallas import tpu as pltpu
from jax.sharding import Mesh, PartitionSpec as P

NORM_EPS = 1e-5
MESH_ID = pl.DeviceIdType.MESH

O_A, O_B, R_B, L_A, F_A, F_B, R_A, L_B = range(8)
UNITS = 8


def rms_norm(stream, norm_row):
    widened = stream.astype(jnp.float32)
    inv_rms = lax.rsqrt(jnp.mean(widened * widened, axis=-1, keepdims=True) + NORM_EPS)
    return (widened * inv_rms * norm_row).astype(jnp.bfloat16)


def dense_gates(hidden, router_l, routes_l):
    experts = router_l.shape[1]
    logits = jnp.dot(hidden, router_l, preferred_element_type=jnp.float32)
    ids = jnp.arange(experts, dtype=routes_l.dtype)
    chosen = jnp.any(routes_l[:, :, None] == ids[None, None, :], axis=1)
    top = jnp.max(jnp.where(chosen, logits, -jnp.inf), axis=-1, keepdims=True)
    weight = jnp.where(chosen, jnp.exp(jnp.where(chosen, logits - top, 0.0)), 0.0)
    gates = weight / jnp.sum(weight, axis=-1, keepdims=True)
    return jnp.where(chosen, gates, -1.0).T


def layer_kernel(first, ring_shape, *refs):
    if first:
        (h_ref, g_ref, gate_ref, up_ref, down_ref, x_ref, out_ref, next_ref, h_all, g_all, w_v, acc, pair_in, ring_in,
         own_sem, ag_send, ag_recv, agp_send, agp_recv, pair_send, pair_recv, ring_send, ring_recv,
         pre_own, pre_send, pre_recv, wr_send, wr_recv) = refs
    else:
        (h_ref, g_ref, w_ref, x_ref, out_ref, h_all, g_all, w_v, acc, pair_in, ring_in,
         own_sem, ag_send, ag_recv, agp_send, agp_recv, pair_send, pair_recv, ring_send, ring_recv, w_sem) = refs
    half, d_model = h_all.shape[1] // 2, h_all.shape[2]
    n_exp = w_v.shape[0]
    n_z, n_y, n_x = ring_shape
    with_ring = n_z == 4 and n_y == 4
    ep, x = lax.axis_index("ep"), lax.axis_index("x")
    z, y = lax.axis_index("z"), lax.axis_index("y")
    right = {"x": lax.rem(x + 1, n_x)}
    left = {"x": lax.rem(x + n_x - 1, n_x)}
    partner = {"ep": 1 - ep}
    group = ep * n_x + x

    def remote(src, dst, send, recv, peer):
        return pltpu.make_async_remote_copy(src, dst, send, recv, device_id=peer, device_id_type=MESH_ID)

    peers = [right, left, partner]
    if first:
        peers.append({"x": lax.rem(x + 2, n_x)})
        if with_ring:
            for axis, pos in (("z", z), ("y", y)):
                peers += [{axis: lax.rem(pos + 1, 4)}, {axis: lax.rem(pos + 3, 4)}]
    barrier = pltpu.get_barrier_semaphore()
    for peer in peers:
        pl.semaphore_signal(barrier, inc=1, device_id=peer, device_id_type=MESH_ID)

    own = []
    for unit in (O_A, O_B):
        rows = pl.ds((unit - O_A) * half, half)
        own.append(pltpu.make_async_copy(h_ref.at[rows], h_all.at[unit, pl.ds(0, half)], own_sem.at[2 * unit]))
        own.append(pltpu.make_async_copy(g_ref.at[:, rows], g_all.at[unit, 0], own_sem.at[2 * unit + 1]))

    if first:
        sources = (gate_ref, up_ref, down_ref)
        targets = (w_v, next_ref)

        def pre_local(layer, m):
            return pltpu.make_async_copy(
                sources[m].at[layer, pl.ds(x * n_exp, n_exp)], targets[layer].at[:, m, z, y, x],
                pre_own.at[layer * 3 + m])

        def pre_copy(layer, m, k):
            there = lax.rem(x + k, n_x)
            idx = (layer * 3 + m) * 3 + k - 1
            return remote(sources[m].at[layer, pl.ds(there * n_exp, n_exp)], targets[layer].at[:, m, z, y, x],
                          pre_send.at[idx], pre_recv.at[idx], {"x": there})

        def ring_copy(layer, r, m, p):
            buf = targets[layer]
            step = 1 if p % 2 == 0 else -1
            along_z = (r < 3) == (p < 2)
            pos = z if along_z else y
            i = lax.rem(pos + 4 - step * (r % 3), 4)
            if r < 3:
                piece = buf.at[p, m, i, y] if along_z else buf.at[p, m, z, i]
            else:
                piece = buf.at[p, m, i] if along_z else buf.at[p, m, :, i]
            idx = ((layer * 6 + r) * 3 + m) * 4 + p
            peer = {"z" if along_z else "y": lax.rem(pos + 4 + step, 4)}
            return remote(piece, piece, wr_send.at[idx], wr_recv.at[idx], peer)

        def pre_start(layer):
            for m in range(3):
                for k in (1, 3, 2):
                    pre_copy(layer, m, k).start()
                pre_local(layer, m).start()

        def pre_wait(layer, m):
            pre_local(layer, m).wait()
            for k in (1, 3, 2):
                pre_copy(layer, m, k).wait_recv()

        def ring_event(layer, r, m):
            if r == 0:
                pre_wait(layer, m)
            if with_ring:
                for p in range(4):
                    if r > 0:
                        ring_copy(layer, r - 1, m, p).wait_recv()
                    if r < 6:
                        ring_copy(layer, r, m, p).start()

        def ring_round(layer, r):
            for m in range(3):
                ring_event(layer, r, m)
    else:
        loads = [pltpu.make_async_copy(w_ref.at[e], w_v.at[e], w_sem.at[e]) for e in range(n_exp)]

    def pair_copy(unit):
        return (
            remote(h_all.at[unit, pl.ds(0, half)], h_all.at[unit, pl.ds(half, half)],
                   agp_send.at[2 * unit], agp_recv.at[2 * unit], partner),
            remote(g_all.at[unit, 0], g_all.at[unit, 1],
                   agp_send.at[2 * unit + 1], agp_recv.at[2 * unit + 1], partner),
        )

    moves = {
        L_A: (0, O_A, right), R_B: (1, O_B, left),
        L_B: (2, O_B, right), R_A: (3, O_A, left),
        F_A: (4, L_A, right), F_B: (5, R_B, left),
    }

    def ring_gather(dst):
        idx, src, peer = moves[dst]
        return (
            remote(h_all.at[src, pl.ds(0, half)], h_all.at[dst, pl.ds(0, half)],
                   ag_send.at[2 * idx], ag_recv.at[2 * idx], peer),
            remote(g_all.at[src, 0], g_all.at[dst, 0], ag_send.at[2 * idx + 1], ag_recv.at[2 * idx + 1], peer),
        )

    def start(copies):
        for copy in copies:
            copy.start()

    def wait_recv(copies):
        for copy in copies:
            copy.wait_recv()

    def wait_send(copies):
        for copy in copies:
            copy.wait_send()

    def reduce_pair(unit):
        return remote(acc.at[unit, pl.ds(half, half)], pair_in.at[unit],
                      pair_send.at[unit], pair_recv.at[unit], partner)

    sums = {R_B: (0, right), F_A: (1, right), R_A: (2, right), L_A: (3, left), F_B: (4, left), L_B: (5, left)}

    def reduce_ring(unit):
        slot, peer = sums[unit]
        return remote(acc.at[unit, pl.ds(0, half)], ring_in.at[slot], ring_send.at[slot], ring_recv.at[slot], peer)

    def add_pair(unit):
        reduce_pair(unit).wait_recv()
        acc[unit, 0:half, :] += pair_in[unit]

    def add_far(unit, far):
        reduce_ring(far).wait_recv()
        acc[unit, 0:half, :] += ring_in[sums[far][0]]

    def arrive(*units):
        for unit in units:
            wait_recv(ring_gather(unit))
            if unit == L_A:
                start(ring_gather(F_A))
            if unit == R_B:
                start(ring_gather(F_B))
            start(pair_copy(unit))

    for copy in own:
        copy.start()
    if not first:
        start(loads)
    for copy in own:
        copy.wait()
    pl.semaphore_wait(barrier, len(peers))
    if first:
        pre_start(0)
    start(ring_gather(L_A))
    start(ring_gather(R_B))
    for unit in (O_A, O_B):
        start(pair_copy(unit))
    if first:
        start(ring_gather(L_B))
        start(ring_gather(R_A))

    plan = {}

    def at(t, action, *args):
        plan.setdefault(t, []).append((action, args))

    if first:
        order = (F_A, F_B, R_B, L_A, R_A, L_B, O_A, O_B)
        for r in range(3):
            ring_round(0, r)
        arrive(L_A, R_B)
        pre_start(1)
        ring_round(0, 3)
        ring_round(0, 4)
        arrive(L_B, R_A)
        ring_round(0, 5)
        arrive(F_A, F_B)
        ring_round(1, 0)
        ring_round(0, 6)
        for unit in range(UNITS):
            wait_recv(pair_copy(unit))
        times = {1: (2, 2, 3), 2: (4, 5, 6), 3: (7, 8, 9), 4: (15, 18, 20), 5: (25, 28, 31)}
        for r, when in times.items():
            for m in range(3):
                at(when[m], ring_event, 1, r, m)
    else:
        order = tuple(range(UNITS))
        for e in range(n_exp):
            at(e, loads[e].wait)
        at(4, arrive, L_A, R_B)
        at(4, start, ring_gather(L_B))
        at(4, start, ring_gather(R_A))
        at(13, arrive, F_A, F_B)
        at(20, arrive, L_B, R_A)
        for k, unit in enumerate(order):
            at(n_exp * k, lambda unit=unit: wait_recv(pair_copy(unit)))

    steps = UNITS * n_exp
    tail = []
    for k, unit in enumerate(order):
        done = n_exp * (k + 1)
        at(done, lambda unit=unit: reduce_pair(unit).start())
        at(done + 2, add_pair, unit)
        if unit in (R_B, L_A, F_A, F_B):
            at(done + 3, lambda unit=unit: reduce_ring(unit).start())
    if first:
        at(27, add_far, R_A, F_A)
        at(28, lambda: reduce_ring(R_A).start())
        at(29, add_far, L_B, F_B)
        at(30, lambda: reduce_ring(L_B).start())
    else:
        at(steps + 6, add_far, R_A, F_A)
        at(steps + 6, lambda: reduce_ring(R_A).start())
        at(steps + 7, add_far, L_B, F_B)
        at(steps + 7, lambda: reduce_ring(L_B).start())

    def step_fn(step, carry):
        for t in sorted(plan):
            if t < steps:
                @pl.when(step == t)
                def _():
                    for action, args in plan[t]:
                        action(*args)

        k, e = step // n_exp, step % n_exp
        unit = k
        if first:
            unit = jnp.where(k < 2, k + F_A, jnp.where(k < 4, k, jnp.where(k < 6, k + 2, k - 6)))
        tokens = h_all[unit]
        gate_w = w_v[e, 0].reshape(-1, d_model)
        up_w = w_v[e, 1].reshape(-1, d_model)
        down_w = w_v[e, 2].reshape(-1, d_model)
        d_ff = gate_w.shape[0]
        inner = []
        for f in range(0, d_ff, 256):
            nt = (((1,), (1,)), ((), ()))
            u = lax.dot_general(tokens, gate_w[f:f + 256], nt, preferred_element_type=jnp.float32)
            v = lax.dot_general(tokens, up_w[f:f + 256], nt, preferred_element_type=jnp.float32)
            inner.append((jax.nn.silu(u) * v).astype(jnp.bfloat16))
        inner = jnp.concatenate(inner, axis=1)
        row = group * n_exp + e
        gate_cols = []
        for s in range(2):
            gates = g_all[unit, s, pl.ds(row, 1), :]
            gate_cols.append(jnp.broadcast_to(gates, (128, half)).T)
        gate_b = jnp.concatenate(gate_cols, axis=0)
        gate_b = jnp.concatenate([gate_b, gate_b], axis=1)
        start_sum = e == 0
        for c in range(0, d_model, 256):
            o = jnp.dot(inner, down_w[:, c:c + 256], preferred_element_type=jnp.float32)
            o = o.astype(jnp.bfloat16).astype(jnp.float32)
            part = jnp.where(gate_b >= 0.0, gate_b * o, 0.0)
            prev = jnp.where(start_sum, 0.0, acc[unit, :, c:c + 256])
            acc[unit, :, c:c + 256] = prev + part
        return carry

    lax.fori_loop(0, steps, step_fn, 0)

    for t in sorted(plan):
        if t >= steps:
            for action, args in plan[t]:
                action(*args)

    reduce_ring(R_B).wait_recv()
    reduce_ring(L_A).wait_recv()
    acc[O_B, 0:half, :] += x_ref[half:, :].astype(jnp.float32) + ring_in[0]
    acc[O_A, 0:half, :] += x_ref[:half, :].astype(jnp.float32) + ring_in[3]
    if first:
        ring_round(1, 6)
    reduce_ring(R_A).wait_recv()
    out_ref[0:half, :] = (acc[O_A, 0:half, :] + ring_in[2]).astype(out_ref.dtype)
    reduce_ring(L_B).wait_recv()
    out_ref[half:, :] = (acc[O_B, 0:half, :] + ring_in[5]).astype(out_ref.dtype)

    for unit in range(UNITS):
        wait_send(pair_copy(unit))
        reduce_pair(unit).wait_send()
        if unit in moves:
            wait_send(ring_gather(unit))
        if unit in sums:
            reduce_ring(unit).wait_send()
    if first:
        for layer in range(2):
            for m in range(3):
                for k in (1, 2, 3):
                    pre_copy(layer, m, k).wait_send()
                if with_ring:
                    for r in range(6):
                        for p in range(4):
                            ring_copy(layer, r, m, p).wait_send()


def moe_layer(first, ring_shape, hidden, gates, weights, stream):
    tok_dev, d_model = hidden.shape
    half = tok_dev // 2
    n_z, n_y, n_x = ring_shape
    vmem = pl.BlockSpec(memory_space=pltpu.VMEM)
    hbm = pl.BlockSpec(memory_space=pl.ANY)
    dma = pltpu.SemaphoreType.DMA
    if first:
        n_exp, f_dev = weights[0].shape[1] // n_x, weights[0].shape[2]
        w_shape = (n_exp, 3, n_z, n_y, n_x, f_dev, d_model)
    else:
        w_shape = weights[0].shape
        n_exp = w_shape[0]
    out_shape = [jax.ShapeDtypeStruct(stream.shape, stream.dtype)]
    out_specs = [vmem]
    extra = [dma((n_exp,))]
    if first:
        out_shape.append(jax.ShapeDtypeStruct(w_shape, jnp.bfloat16))
        out_specs.append(hbm)
        extra = [dma((6,)), dma((18,)), dma((18,)), dma((144,)), dma((144,))]
    return pl.pallas_call(
        functools.partial(layer_kernel, first, ring_shape),
        name="moe_first" if first else "moe_second",
        out_shape=out_shape,
        in_specs=[hbm, hbm] + [hbm] * len(weights) + [vmem],
        out_specs=out_specs,
        scratch_shapes=[
            pltpu.VMEM((UNITS, tok_dev, d_model), jnp.bfloat16),
            pltpu.VMEM((UNITS, 2, gates.shape[0], half), jnp.float32),
            pltpu.VMEM(w_shape, jnp.bfloat16),
            pltpu.VMEM((UNITS, tok_dev, d_model), jnp.float32),
            pltpu.VMEM((UNITS, half, d_model), jnp.float32),
            pltpu.VMEM((6, half, d_model), jnp.float32),
            dma((4,)),
            dma((12,)), dma((12,)), dma((16,)), dma((16,)), dma((8,)), dma((8,)), dma((6,)), dma((6,)),
        ] + extra,
        compiler_params=pltpu.CompilerParams(
            collective_id=0 if first else 1, has_side_effects=True, vmem_limit_bytes=67043328),
        cost_estimate=pl.CostEstimate(flops=52 * 10**9, bytes_accessed=16 * 2**20, transcendentals=0),
    )(hidden, gates, *weights, stream)


def solution(mesh):
    n_x = 4
    n_y = min(4, mesh.shape["fsdp"] // n_x)
    devices = mesh.devices.reshape(mesh.shape["rep"], mesh.shape["ep"], -1, n_y, n_x)
    cells = Mesh(devices, ("rep", "ep", "z", "y", "x"))
    ring_shape = devices.shape[2:]
    fsdp = ("z", "y", "x")
    token_spec = P(("rep", "ep") + fsdp, None)
    expert_in_spec = P(None, "ep", None, fsdp)
    expert_out_spec = P(None, "ep", fsdp, None)
    route_spec = P(None, ("rep", "ep") + fsdp, None)

    def device_step(x_in, norm_w, router_w, gate_w, up_w, down_w, routes):
        shards = (gate_w.transpose(0, 1, 3, 2), up_w.transpose(0, 1, 3, 2), down_w)
        hidden = rms_norm(x_in, norm_w[0])
        gates = dense_gates(hidden, router_w[0], routes[0])
        stream, weights = moe_layer(True, ring_shape, hidden, gates, shards, x_in)
        hidden = rms_norm(stream, norm_w[1])
        gates = dense_gates(hidden, router_w[1], routes[1])
        return moe_layer(False, ring_shape, hidden, gates, (weights,), stream)[0]

    return jax.shard_map(device_step, mesh=cells,
                         in_specs=(token_spec, P(), P(), expert_in_spec, expert_in_spec, expert_out_spec, route_spec),
                         out_specs=token_spec, check_vma=False)
```

```python
import functools

import jax
import jax.numpy as jnp
from jax import lax
from jax.experimental import pallas as pl
from jax.experimental.pallas import tpu as pltpu
from jax.sharding import Mesh, PartitionSpec as P

NORM_EPS = 1e-5
MESH_ID = pl.DeviceIdType.MESH

OWN, NEAR, FAR, MORE = range(4)
UNITS = 8


def rms_norm(stream, norm_row):
    widened = stream.astype(jnp.float32)
    inv_rms = lax.rsqrt(jnp.mean(widened * widened, axis=-1, keepdims=True) + NORM_EPS)
    return (widened * inv_rms * norm_row).astype(jnp.bfloat16)


def dense_gates(hidden, router_l, routes_l):
    experts = router_l.shape[1]
    logits = jnp.dot(hidden, router_l, preferred_element_type=jnp.float32)
    ids = jnp.arange(experts, dtype=routes_l.dtype)
    chosen = jnp.any(routes_l[:, :, None] == ids[None, None, :], axis=1)
    top = jnp.max(jnp.where(chosen, logits, -jnp.inf), axis=-1, keepdims=True)
    weight = jnp.where(chosen, jnp.exp(jnp.where(chosen, logits - top, 0.0)), 0.0)
    gates = weight / jnp.sum(weight, axis=-1, keepdims=True)
    return jnp.where(chosen, gates, -1.0).T


def layer_kernel(first, ring_shape, *refs):
    if first:
        (h_ref, g_ref, gate_ref, up_ref, down_ref, x_ref, out_ref, next_ref, h_all, g_all, w_v, acc, pair_in, ring_in,
         own_sem, ag_send, ag_recv, agp_send, agp_recv, pair_send, pair_recv, ring_send, ring_recv,
         pre_own, pre_send, pre_recv, wr_send, wr_recv) = refs
    else:
        (h_ref, g_ref, w_ref, x_ref, out_ref, h_all, g_all, w_v, acc, pair_in, ring_in,
         own_sem, ag_send, ag_recv, agp_send, agp_recv, pair_send, pair_recv, ring_send, ring_recv, w_sem) = refs
    part, d_model = h_all.shape[3], h_all.shape[4]
    n_exp = w_v.shape[0]
    n_z, n_y, n_x = ring_shape
    ep, x = lax.axis_index("ep"), lax.axis_index("x")
    z, y = lax.axis_index("z"), lax.axis_index("y")
    partner = {"ep": 1 - ep}
    owner = lax.rem(x + y, 4)
    group = ep * 4 + owner

    def remote(src, dst, send, recv, peer):
        return pltpu.make_async_remote_copy(src, dst, send, recv, device_id=peer, device_id_type=MESH_ID)

    def beside(axis, stream):
        move = 1 + 2 * stream
        return {"x": lax.rem(x + (1 - axis) * move, 4), "y": lax.rem(y + axis * move, 4)}

    def diagonal(step):
        return {"x": lax.rem(x + 4 - step, 4), "y": lax.rem(y + 4 + step, 4)}

    peers = [beside(axis, stream) for axis in range(2) for stream in range(2)] + [partner]
    if first:
        peers.append({"x": lax.rem(x + 2, 4)})
        peers += [diagonal(1), diagonal(-1)]
        if n_z > 1:
            peers += [{"z": lax.rem(z + 1, n_z)}, {"z": lax.rem(z + n_z - 1, n_z)}]
    barrier = pltpu.get_barrier_semaphore()
    for peer in peers:
        pl.semaphore_signal(barrier, inc=1, device_id=peer, device_id_type=MESH_ID)

    own = []
    for axis in range(2):
        for t in range(2):
            idx = 2 * axis + t
            rows = pl.ds(idx * part, part)
            own.append(pltpu.make_async_copy(h_ref.at[rows], h_all.at[axis, t, 0], own_sem.at[2 * idx]))
            own.append(pltpu.make_async_copy(g_ref.at[:, rows], g_all.at[axis, t, 0], own_sem.at[2 * idx + 1]))

    if first:
        sources = (gate_ref, up_ref, down_ref)
        targets = (w_v, next_ref)

        def pre_local(layer, m):
            return pltpu.make_async_copy(
                sources[m].at[layer, pl.ds(owner * n_exp, n_exp)], targets[layer].at[:, m, z, y, x],
                pre_own.at[layer * 3 + m])

        def pre_copy(layer, m, k):
            idx = (layer * 3 + m) * 3 + k - 1
            return remote(sources[m].at[layer, pl.ds(lax.rem(owner + k, 4) * n_exp, n_exp)],
                          targets[layer].at[:, m, z, y, x],
                          pre_send.at[idx], pre_recv.at[idx], {"x": lax.rem(x + k, 4)})

        def z_first(m, p):
            return m == p // 2

        def rounds(m, p):
            sizes = (n_z, n_y) if z_first(m, p) else (n_y, n_z)
            return [r for r in range(6) if sizes[r // 3] > 1]

        def ring_copy(layer, r, m, p):
            buf = targets[layer]
            step = 1 if p % 2 == 0 else -1
            along_z = (r < 3) == z_first(m, p)
            pos = z if along_z else y
            i = lax.rem(pos + 4 - step * (r % 3), 4)
            if r < 3:
                piece = buf.at[p, m, i, y] if along_z else buf.at[p, m, z, i]
            else:
                piece = buf.at[p, m, i] if along_z else buf.at[p, m, :, i]
            idx = ((layer * 6 + r) * 3 + m) * 4 + p
            peer = {"z": lax.rem(z + 4 + step, 4)} if along_z else diagonal(step)
            return remote(piece, piece, wr_send.at[idx], wr_recv.at[idx], peer)

        def pre_start(layer):
            for m in range(3):
                for k in (1, 3, 2):
                    pre_copy(layer, m, k).start()
                pre_local(layer, m).start()

        def pre_wait(layer, m):
            pre_local(layer, m).wait()
            for k in (1, 3, 2):
                pre_copy(layer, m, k).wait_recv()

        def ring_event(layer, r, m):
            with jax.named_scope(f"w{layer}r{r}m{m}"):
                if r == 0:
                    pre_wait(layer, m)
                for p in range(4):
                    before = [q for q in rounds(m, p) if q < r]
                    if r in rounds(m, p) or r == 6:
                        if before:
                            ring_copy(layer, before[-1], m, p).wait_recv()
                    if r in rounds(m, p):
                        ring_copy(layer, r, m, p).start()

        def ring_round(layer, r):
            for m in range(3):
                ring_event(layer, r, m)
    else:
        loads = [pltpu.make_async_copy(w_ref.at[e], w_v.at[e], w_sem.at[e]) for e in range(n_exp)]

    def pair_copy(unit):
        return (
            remote(h_all.at[unit, :, 0], h_all.at[unit, :, 1], agp_send.at[unit], agp_recv.at[unit], partner),
            remote(g_all.at[unit, :, 0], g_all.at[unit, :, 1], agp_send.at[8 + unit], agp_recv.at[8 + unit], partner),
        )

    def gather(axis, kind, t):
        src_kind, src_t, to = {
            (NEAR, 1): (OWN, 0, 0), (MORE, 1): (OWN, 1, 0), (FAR, 0): (NEAR, 1, 0),
            (NEAR, 0): (OWN, 1, 1), (MORE, 0): (OWN, 0, 1), (FAR, 1): (NEAR, 0, 1),
        }[kind, t]
        src, dst = 2 * src_kind + axis, 2 * kind + axis
        idx = 2 * (dst - 2) + t
        peer = beside(axis, to)
        return (
            remote(h_all.at[src, src_t, 0], h_all.at[dst, t, 0], ag_send.at[idx], ag_recv.at[idx], peer),
            remote(g_all.at[src, src_t, 0], g_all.at[dst, t, 0], ag_send.at[12 + idx], ag_recv.at[12 + idx], peer),
        )

    def start(copies):
        for copy in copies:
            copy.start()

    def wait_recv(copies):
        for copy in copies:
            copy.wait_recv()

    def wait_send(copies):
        for copy in copies:
            copy.wait_send()

    def gather_start(kind):
        for axis in range(2):
            for t in range(2):
                start(gather(axis, kind, t))

    def arrive(kind):
        with jax.named_scope(f"arr{kind}"):
            for axis in range(2):
                for t in range(2):
                    wait_recv(gather(axis, kind, t))
                    if kind == NEAR:
                        start(gather(axis, FAR, 1 - t))
                start(pair_copy(2 * kind + axis))

    def reduce_pair(unit):
        return remote(acc.at[unit, :, 1], pair_in.at[unit], pair_send.at[unit], pair_recv.at[unit], partner)

    def reduce_ring(unit, t):
        slot = 2 * (unit - 2) + t
        return remote(acc.at[unit, t, 0], ring_in.at[slot], ring_send.at[slot], ring_recv.at[slot],
                      beside(unit % 2, t))

    def add_pair(unit):
        with jax.named_scope("pairw"):
            reduce_pair(unit).wait_recv()
        acc[unit, :, 0] += pair_in[unit]

    def add_more(unit):
        with jax.named_scope("morew"):
            reduce_pair(unit).wait_recv()
            far = unit - 2 * (MORE - FAR)
            for t in range(2):
                reduce_ring(far, t).wait_recv()
        for t in range(2):
            acc[unit, t, 0] += pair_in[unit, t] + ring_in[2 * (far - 2) + t]

    def ring_start(unit):
        for t in range(2):
            reduce_ring(unit, t).start()

    for copy in own:
        copy.start()
    if not first:
        start(loads)
    for copy in own:
        copy.wait()
    with jax.named_scope("barrier"):
        pl.semaphore_wait(barrier, len(peers))
    if first:
        pre_start(0)
    gather_start(NEAR)
    for axis in range(2):
        start(pair_copy(axis))
    gather_start(MORE)

    steps = UNITS * n_exp
    plan = {}

    def at(t, action, *args):
        plan.setdefault(t, []).append((action, args))

    if first:
        kinds = (FAR, NEAR, MORE, OWN)
        for r in range(3):
            ring_round(0, r)
        arrive(NEAR)
        pre_start(1)
        ring_round(0, 3)
        arrive(MORE)
        ring_round(0, 4)
        arrive(FAR)
        ring_round(0, 5)
        ring_round(1, 0)
        ring_round(0, 6)
        for unit in range(UNITS):
            wait_recv(pair_copy(unit))
        times = {1: (2, 2, 3), 2: (5, 5, 6), 3: (8, 8, 9), 4: (16, 18, 20), 5: (28, 30, 31)}
        for r, when in times.items():
            for m in range(3):
                at(when[m], ring_event, 1, r, m)
    else:
        kinds = (OWN, NEAR, FAR, MORE)
        for e in range(n_exp):
            at(e, loads[e].wait)
        at(3, arrive, NEAR)
        at(6, arrive, MORE)
        at(9, arrive, FAR)

    def unit_of(k):
        turn, axis = k // 2, k % 2
        kind = turn
        if first:
            kind = jnp.where(turn == 0, FAR, jnp.where(turn == 1, NEAR, jnp.where(turn == 2, MORE, OWN)))
        return 2 * kind + axis

    more_turn, own_turn = kinds.index(MORE), kinds.index(OWN)

    def finished(k, e):
        before = unit_of(k - 1)
        turn = (k - 1) // 2

        @pl.when(e == 0)
        def _():
            reduce_pair(before).start()

        @pl.when((e == 2) & (turn != more_turn))
        def _():
            add_pair(before)

        @pl.when((e == 3) & (turn != own_turn) & (turn != more_turn))
        def _():
            ring_start(before)

        if first:
            late = unit_of(k - 2)

            @pl.when((e == 2) & ((k - 2) // 2 == more_turn) & (k >= 2))
            def _():
                add_more(late)

            @pl.when((e == 3) & ((k - 2) // 2 == more_turn) & (k >= 2))
            def _():
                ring_start(late)

    def step_fn(step, carry):
        k, e = step // n_exp, step % n_exp
        for t in sorted(plan):
            @pl.when(step == t)
            def _():
                for action, args in plan[t]:
                    action(*args)

        @pl.when(k >= 1)
        def _():
            finished(k, e)

        unit = unit_of(k)
        if not first:
            @pl.when(e == 0)
            def _():
                wait_recv(pair_copy(unit))

        with jax.named_scope("load"):
            tokens = h_all[unit].reshape(-1, d_model)
        gate_w = w_v[e, 0].reshape(-1, d_model)
        up_w = w_v[e, 1].reshape(-1, d_model)
        down_w = w_v[e, 2].reshape(-1, d_model)
        d_ff = gate_w.shape[0]
        inner = []
        for f in range(0, d_ff, 256):
            nt = (((1,), (1,)), ((), ()))
            u = lax.dot_general(tokens, gate_w[f:f + 256], nt, preferred_element_type=jnp.float32)
            v = lax.dot_general(tokens, up_w[f:f + 256], nt, preferred_element_type=jnp.float32)
            inner.append((jax.nn.silu(u) * v).astype(jnp.bfloat16))
        inner = jnp.concatenate(inner, axis=1)
        row = group * n_exp + e
        gate_cols = []
        for t in range(2):
            for s in range(2):
                gates = g_all[unit, t, s, pl.ds(row, 1), :]
                gate_cols.append(jnp.broadcast_to(gates, (128, part)).T)
        gate_b = jnp.concatenate(gate_cols, axis=0)
        gate_b = jnp.concatenate([gate_b, gate_b], axis=1)
        start_sum = e == 0
        for c in range(0, d_model, 256):
            o = jnp.dot(inner, down_w[:, c:c + 256], preferred_element_type=jnp.float32)
            o = o.astype(jnp.bfloat16).astype(jnp.float32)
            new = jnp.where(gate_b >= 0.0, gate_b * o, 0.0).reshape(2, 2, part, 256)
            prev = jnp.where(start_sum, 0.0, acc[unit, :, :, :, c:c + 256])
            acc[unit, :, :, :, c:c + 256] = prev + new
        return carry

    lax.fori_loop(0, steps, step_fn, 0)

    last = 2 * kinds[3] + 1
    reduce_pair(last).start()
    if first:
        add_pair(last)
    else:
        add_more(last - 1)
        ring_start(last - 1)
        add_more(last)
        ring_start(last)

    for axis in range(2):
        near, more = 2 * NEAR + axis, 2 * MORE + axis
        for t in range(2):
            with jax.named_scope("fin1"):
                reduce_ring(near, 1 - t).wait_recv()
            rows = pl.ds((2 * axis + t) * part, part)
            acc[axis, t, 0] += x_ref[rows, :].astype(jnp.float32) + ring_in[2 * (near - 2) + 1 - t]
    if first:
        ring_round(1, 6)
    for axis in range(2):
        more = 2 * MORE + axis
        for t in range(2):
            with jax.named_scope("fin2"):
                reduce_ring(more, t).wait_recv()
            rows = pl.ds((2 * axis + t) * part, part)
            out_ref[rows, :] = (acc[axis, t, 0] + ring_in[2 * (more - 2) + t]).astype(out_ref.dtype)

    for unit in range(UNITS):
        wait_send(pair_copy(unit))
        reduce_pair(unit).wait_send()
        if unit >= 2:
            for t in range(2):
                wait_send(gather(unit % 2, unit // 2, t))
                reduce_ring(unit, t).wait_send()
    if first:
        for layer in range(2):
            for m in range(3):
                for k in (1, 2, 3):
                    pre_copy(layer, m, k).wait_send()
                for p in range(4):
                    for r in rounds(m, p):
                        ring_copy(layer, r, m, p).wait_send()


def moe_layer(first, ring_shape, hidden, gates, weights, stream):
    tok_dev, d_model = hidden.shape
    part = tok_dev // 4
    n_z, n_y, n_x = ring_shape
    vmem = pl.BlockSpec(memory_space=pltpu.VMEM)
    hbm = pl.BlockSpec(memory_space=pl.ANY)
    dma = pltpu.SemaphoreType.DMA
    if first:
        n_exp, f_dev = weights[0].shape[1] // n_x, weights[0].shape[2]
        w_shape = (n_exp, 3, n_z, n_y, n_x, f_dev, d_model)
    else:
        w_shape = weights[0].shape
        n_exp = w_shape[0]
    out_shape = [jax.ShapeDtypeStruct(stream.shape, stream.dtype)]
    out_specs = [vmem]
    extra = [dma((n_exp,))]
    if first:
        out_shape.append(jax.ShapeDtypeStruct(w_shape, jnp.bfloat16))
        out_specs.append(hbm)
        extra = [dma((6,)), dma((18,)), dma((18,)), dma((144,)), dma((144,))]
    return pl.pallas_call(
        functools.partial(layer_kernel, first, ring_shape),
        name="moe_first" if first else "moe_second",
        out_shape=out_shape,
        in_specs=[hbm, hbm] + [hbm] * len(weights) + [vmem],
        out_specs=out_specs,
        scratch_shapes=[
            pltpu.VMEM((UNITS, 2, 2, part, d_model), jnp.bfloat16),
            pltpu.VMEM((UNITS, 2, 2, gates.shape[0], part), jnp.float32),
            pltpu.VMEM(w_shape, jnp.bfloat16),
            pltpu.VMEM((UNITS, 2, 2, part, d_model), jnp.float32),
            pltpu.VMEM((UNITS, 2, part, d_model), jnp.float32),
            pltpu.VMEM((12, part, d_model), jnp.float32),
            dma((8,)),
            dma((24,)), dma((24,)), dma((16,)), dma((16,)), dma((8,)), dma((8,)), dma((12,)), dma((12,)),
        ] + extra,
        compiler_params=pltpu.CompilerParams(
            collective_id=0 if first else 1, has_side_effects=True, vmem_limit_bytes=67043328),
        cost_estimate=pl.CostEstimate(flops=52 * 10**9, bytes_accessed=16 * 2**20, transcendentals=0),
    )(hidden, gates, *weights, stream)


def solution(mesh):
    n_x = 4
    n_y = min(4, mesh.shape["fsdp"] // n_x)
    devices = mesh.devices.reshape(mesh.shape["rep"], mesh.shape["ep"], -1, n_y, n_x)
    cells = Mesh(devices, ("rep", "ep", "z", "y", "x"))
    ring_shape = devices.shape[2:]
    fsdp = ("z", "y", "x")
    token_spec = P(("rep", "ep") + fsdp, None)
    expert_in_spec = P(None, "ep", None, fsdp)
    expert_out_spec = P(None, "ep", fsdp, None)
    route_spec = P(None, ("rep", "ep") + fsdp, None)

    def device_step(x_in, norm_w, router_w, gate_w, up_w, down_w, routes):
        shards = (gate_w.transpose(0, 1, 3, 2), up_w.transpose(0, 1, 3, 2), down_w)
        hidden = rms_norm(x_in, norm_w[0])
        gates = dense_gates(hidden, router_w[0], routes[0])
        stream, weights = moe_layer(True, ring_shape, hidden, gates, shards, x_in)
        hidden = rms_norm(stream, norm_w[1])
        gates = dense_gates(hidden, router_w[1], routes[1])
        return moe_layer(False, ring_shape, hidden, gates, (weights,), stream)[0]

    return jax.shard_map(device_step, mesh=cells,
                         in_specs=(token_spec, P(), P(), expert_in_spec, expert_in_spec, expert_out_spec, route_spec),
                         out_specs=token_spec, check_vma=False)
```

```python
import functools

import jax
import jax.numpy as jnp
from jax import lax
from jax.experimental import pallas as pl
from jax.experimental.pallas import tpu as pltpu
from jax.sharding import Mesh, PartitionSpec as P

NORM_EPS = 1e-5
MESH_ID = pl.DeviceIdType.MESH

OWN, NEAR, FAR, MORE = range(4)
UNITS = 8
TWO_RINGS = True
W1_TIMES = {4: (13, 17, 21), 5: (25, 29, 31)}


def kernel(ring_shape, x_ref, norm_ref, router_ref, routes_ref, gate_ref, up_ref, down_ref, out_ref, next_ref,
           h_all, g_all, w_v, acc, pair_in, ring_in,
           ag_send, ag_recv, agp_send, agp_recv, pair_send, pair_recv, ring_send, ring_recv,
           pre_own, pre_send, pre_recv, wr_send, wr_recv, w_sem, ready):
    part, d_model = h_all.shape[3], h_all.shape[4]
    n_exp = w_v.shape[0]
    n_z, n_y, n_x = ring_shape
    ep, x = lax.axis_index("ep"), lax.axis_index("x")
    z, y = lax.axis_index("z"), lax.axis_index("y")
    partner = {"ep": 1 - ep}
    owners = (x, lax.rem(x + y, 4) if TWO_RINGS else x)
    steps = UNITS * n_exp

    def remote(src, dst, send, recv, peer):
        return pltpu.make_async_remote_copy(src, dst, send, recv, device_id=peer, device_id_type=MESH_ID)

    def beside(layer, axis, stream):
        move = 1 + 2 * stream
        if layer == 0 or not TWO_RINGS:
            return {"x": lax.rem(x + move, 4)}
        return {"x": lax.rem(x + (1 - axis) * move, 4), "y": lax.rem(y + axis * move, 4)}

    def next_row(layer, step):
        if layer == 0 or not TWO_RINGS:
            return {"y": lax.rem(y + 4 + step, 4)}
        return {"x": lax.rem(x + 4 - step, 4), "y": lax.rem(y + 4 + step, 4)}

    token_peers = [beside(0, 0, 0), beside(0, 0, 1), partner]
    if TWO_RINGS:
        token_peers += [beside(1, 1, 0), beside(1, 1, 1)]
    peers = token_peers + [{"x": lax.rem(x + 2, 4)}] + [next_row(1, step) for step in (1, -1)]
    if n_z > 1:
        peers += [{"z": lax.rem(z + 1, n_z)}, {"z": lax.rem(z + n_z - 1, n_z)}]
    barrier = pltpu.get_barrier_semaphore()
    for peer in peers:
        pl.semaphore_signal(barrier, inc=1, device_id=peer, device_id_type=MESH_ID)

    sources = (gate_ref, up_ref, down_ref)
    targets = (w_v, next_ref)

    def pre_local(layer, m):
        return pltpu.make_async_copy(
            sources[m].at[layer, pl.ds(owners[layer] * n_exp, n_exp)], targets[layer].at[:, m, z, y, x],
            pre_own.at[layer * 3 + m])

    def pre_copy(layer, m, k):
        idx = (layer * 3 + m) * 3 + k - 1
        return remote(sources[m].at[layer, pl.ds(lax.rem(owners[layer] + k, 4) * n_exp, n_exp)],
                      targets[layer].at[:, m, z, y, x],
                      pre_send.at[idx], pre_recv.at[idx], {"x": lax.rem(x + k, 4)})

    def z_first(layer, m, p):
        return p < 2 and (layer == 0 or not TWO_RINGS or m == 1)

    def rounds(layer, m, p):
        sizes = (n_z, n_y) if z_first(layer, m, p) else (n_y, n_z)
        return [r for r in range(6) if sizes[r // 3] > 1]

    def ring_copy(layer, r, m, p):
        buf = targets[layer]
        step = 1 if p % 2 == 0 else -1
        along_z = (r < 3) == z_first(layer, m, p)
        pos = z if along_z else y
        i = lax.rem(pos + 4 - step * (r % 3), 4)
        if r < 3:
            piece = buf.at[p, m, i, y] if along_z else buf.at[p, m, z, i]
        else:
            piece = buf.at[p, m, i] if along_z else buf.at[p, m, :, i]
        idx = ((layer * 6 + r) * 3 + m) * 4 + p
        peer = {"z": lax.rem(z + 4 + step, 4)} if along_z else next_row(layer, step)
        return remote(piece, piece, wr_send.at[idx], wr_recv.at[idx], peer)

    def pre_start(layer):
        for m in range(3):
            for k in (1, 3, 2):
                pre_copy(layer, m, k).start()
            pre_local(layer, m).start()

    def ring_event(layer, r, m):
        with jax.named_scope(f"w{layer}r{r}m{m}"):
            if r == 0:
                pre_local(layer, m).wait()
                for k in (1, 3, 2):
                    pre_copy(layer, m, k).wait_recv()
            for p in range(4):
                before = [q for q in rounds(layer, m, p) if q < r]
                if (r in rounds(layer, m, p) or r == 6) and before:
                    ring_copy(layer, before[-1], m, p).wait_recv()
                if r in rounds(layer, m, p):
                    ring_copy(layer, r, m, p).start()

    def ring_round(layer, r):
        for m in range(3):
            ring_event(layer, r, m)

    loads = [pltpu.make_async_copy(next_ref.at[e], w_v.at[e], w_sem.at[e]) for e in range(n_exp)]

    def prepare(layer, stream_ref):
        experts = router_ref.shape[1]
        for axis in range(2):
            for t in range(2):
                rows = pl.ds((2 * axis + t) * part, part)
                wide = stream_ref[rows, :].astype(jnp.float32)
                inv_rms = lax.rsqrt(jnp.mean(wide * wide, axis=-1, keepdims=True) + NORM_EPS)
                hidden = (wide * inv_rms * norm_ref[layer:layer + 1, :]).astype(jnp.bfloat16)
                h_all[axis, t, 0] = hidden
                logits = lax.dot_general(router_ref[layer], hidden, (((1,), (1,)), ((), ())),
                                         preferred_element_type=jnp.float32)
                ids = lax.broadcasted_iota(jnp.int32, (experts, part), 0)
                chosen = ids < 0
                for j in range(routes_ref.shape[1]):
                    chosen |= routes_ref[layer, j:j + 1, (2 * axis + t) * part:(2 * axis + t + 1) * part] == ids
                top = jnp.max(jnp.where(chosen, logits, -jnp.inf), axis=0, keepdims=True)
                weight = jnp.where(chosen, jnp.exp(jnp.where(chosen, logits - top, 0.0)), 0.0)
                gates = weight / jnp.sum(weight, axis=0, keepdims=True)
                g_all[axis, t, 0] = jnp.where(chosen, gates, -1.0)

    def start(copies):
        for copy in copies:
            copy.start()

    def wait_recv(copies):
        for copy in copies:
            copy.wait_recv()

    def wait_send(copies):
        for copy in copies:
            copy.wait_send()

    def run_layer(layer, stream_ref):
        first = layer == 0
        group = ep * 4 + owners[layer]

        def pair_copy(unit):
            return (
                remote(h_all.at[unit, :, 0], h_all.at[unit, :, 1],
                       agp_send.at[layer, unit], agp_recv.at[layer, unit], partner),
                remote(g_all.at[unit, :, 0], g_all.at[unit, :, 1],
                       agp_send.at[layer, 8 + unit], agp_recv.at[layer, 8 + unit], partner),
            )

        def gather(axis, kind, t):
            src_kind, src_t, to = {
                (NEAR, 1): (OWN, 0, 0), (MORE, 1): (OWN, 1, 0), (FAR, 0): (NEAR, 1, 0),
                (NEAR, 0): (OWN, 1, 1), (MORE, 0): (OWN, 0, 1), (FAR, 1): (NEAR, 0, 1),
            }[kind, t]
            src, dst = 2 * src_kind + axis, 2 * kind + axis
            idx = 2 * (dst - 2) + t
            peer = beside(layer, axis, to)
            return (
                remote(h_all.at[src, src_t, 0], h_all.at[dst, t, 0],
                       ag_send.at[layer, idx], ag_recv.at[layer, idx], peer),
                remote(g_all.at[src, src_t, 0], g_all.at[dst, t, 0],
                       ag_send.at[layer, 12 + idx], ag_recv.at[layer, 12 + idx], peer),
            )

        def gather_start(kind):
            for axis in range(2):
                for t in range(2):
                    start(gather(axis, kind, t))

        def arrive(kind):
            with jax.named_scope(f"arr{kind}"):
                for axis in range(2):
                    for t in range(2):
                        wait_recv(gather(axis, kind, t))
                        if kind == NEAR:
                            start(gather(axis, FAR, 1 - t))
                    start(pair_copy(2 * kind + axis))

        def reduce_pair(unit):
            return remote(acc.at[unit, :, 1], pair_in.at[unit],
                          pair_send.at[layer, unit], pair_recv.at[layer, unit], partner)

        def reduce_ring(unit, t):
            slot = 2 * (unit - 2) + t
            return remote(acc.at[unit, t, 0], ring_in.at[slot], ring_send.at[layer, slot], ring_recv.at[layer, slot],
                          beside(layer, unit % 2, t))

        def add_pair(unit):
            with jax.named_scope("pairw"):
                reduce_pair(unit).wait_recv()
            acc[unit, :, 0] += pair_in[unit]

        def add_more(unit):
            with jax.named_scope("morew"):
                reduce_pair(unit).wait_recv()
                far = unit - 2 * (MORE - FAR)
                for t in range(2):
                    reduce_ring(far, t).wait_recv()
            for t in range(2):
                acc[unit, t, 0] += pair_in[unit, t] + ring_in[2 * (far - 2) + t]

        def ring_start(unit):
            for t in range(2):
                reduce_ring(unit, t).start()

        plan = {}

        def at(t, action, *args):
            plan.setdefault(t, []).append((action, args))

        prepare(layer, stream_ref)
        if not first:
            with jax.named_scope("ready"):
                pl.semaphore_wait(ready, len(token_peers))
        gather_start(NEAR)
        for axis in range(2):
            start(pair_copy(axis))
        gather_start(MORE)
        if first:
            for r in range(3):
                ring_round(0, r)
            arrive(NEAR)
            pre_start(1)
            ring_round(0, 3)
            ring_round(0, 4)
            arrive(MORE)
            ring_round(0, 5)
            arrive(FAR)
            ring_round(1, 0)
            ring_round(0, 6)
            for unit in range(UNITS):
                wait_recv(pair_copy(unit))
            for t, r in ((1, 1), (3, 2), (5, 3)):
                at(t, ring_round, 1, r)
            for r, when in W1_TIMES.items():
                for m in range(3):
                    at(when[m], ring_event, 1, r, m)
        else:
            ring_round(1, 6)
            start(loads)
            for e in range(n_exp):
                at(e, loads[e].wait)
            at(3, arrive, NEAR)
            at(6, arrive, MORE)
            at(9, arrive, FAR)

        def unit_of(k):
            if first:
                return jnp.where(k < 2, k + 2 * FAR, jnp.where(k < 4, k, jnp.where(k < 6, k + 2, k - 6)))
            return jnp.where(k == 0, 0, jnp.where(k == UNITS - 1, 1, k + 1))

        def step_fn(step, carry):
            k, e = step // n_exp, step % n_exp
            before, late = unit_of(k - 1), unit_of(k - 2)
            kind, late_kind = before // 2, late // 2

            def planned(e_static):
                for t in sorted(plan):
                    if t % n_exp == e_static:
                        @pl.when(k == t // n_exp)
                        def _():
                            for action, args in plan[t]:
                                action(*args)

            @pl.when(e == 0)
            def _():
                planned(0)

                @pl.when(k >= 1)
                def _():
                    reduce_pair(before).start()

                if not first:
                    wait_recv(pair_copy(unit_of(k)))

            @pl.when(e == 1)
            def _():
                planned(1)

            @pl.when(e == 2)
            def _():
                planned(2)

                @pl.when((k >= 1) & (kind != MORE))
                def _():
                    add_pair(before)

                @pl.when((k >= 2) & (late_kind == MORE) if first else (k >= 1) & (kind == MORE))
                def _():
                    add_more(late if first else before)

            @pl.when(e == 3)
            def _():
                planned(3)

                @pl.when((k >= 1) & (kind != OWN) & ((kind != MORE) if first else True))
                def _():
                    ring_start(before)

                if first:
                    @pl.when((k >= 2) & (late_kind == MORE))
                    def _():
                        ring_start(late)

            unit = unit_of(k)
            with jax.named_scope("load"):
                tokens = h_all[unit].reshape(-1, d_model)
            gate_w = w_v[e, 0].reshape(-1, d_model)
            up_w = w_v[e, 1].reshape(-1, d_model)
            down_w = w_v[e, 2].reshape(-1, d_model)
            d_ff = gate_w.shape[0]
            inner = []
            for f in range(0, d_ff, 256):
                nt = (((1,), (1,)), ((), ()))
                u = lax.dot_general(tokens, gate_w[f:f + 256], nt, preferred_element_type=jnp.float32)
                v = lax.dot_general(tokens, up_w[f:f + 256], nt, preferred_element_type=jnp.float32)
                inner.append((jax.nn.silu(u) * v).astype(jnp.bfloat16))
            inner = jnp.concatenate(inner, axis=1)
            row = group * n_exp + e
            gate_cols = []
            for t in range(2):
                for s in range(2):
                    gates = g_all[unit, t, s, pl.ds(row, 1), :]
                    gate_cols.append(jnp.broadcast_to(gates, (128, part)).T)
            gate_b = jnp.concatenate(gate_cols, axis=0)
            gate_b = jnp.concatenate([gate_b, gate_b], axis=1)
            start_sum = e == 0
            for c in range(0, d_model, 256):
                o = jnp.dot(inner, down_w[:, c:c + 256], preferred_element_type=jnp.float32)
                o = o.astype(jnp.bfloat16).astype(jnp.float32)
                new = jnp.where(gate_b >= 0.0, gate_b * o, 0.0).reshape(2, 2, part, 256)
                prev = jnp.where(start_sum, 0.0, acc[unit, :, :, :, c:c + 256])
                acc[unit, :, :, :, c:c + 256] = prev + new
            return carry

        lax.fori_loop(0, steps, step_fn, 0)
        reduce_pair(1).start()
        add_pair(1)

        for axis in range(2):
            near = 2 * NEAR + axis
            for t in range(2):
                with jax.named_scope("fin1"):
                    reduce_ring(near, 1 - t).wait_recv()
                rows = pl.ds((2 * axis + t) * part, part)
                acc[axis, t, 0] += stream_ref[rows, :].astype(jnp.float32) + ring_in[2 * (near - 2) + 1 - t]
        for axis in range(2):
            more = 2 * MORE + axis
            for t in range(2):
                with jax.named_scope("fin2"):
                    reduce_ring(more, t).wait_recv()
                rows = pl.ds((2 * axis + t) * part, part)
                out_ref[rows, :] = (acc[axis, t, 0] + ring_in[2 * (more - 2) + t]).astype(out_ref.dtype)
        for unit in range(UNITS):
            wait_send(pair_copy(unit))
            reduce_pair(unit).wait_send()
            if unit >= 2:
                for t in range(2):
                    wait_send(gather(unit % 2, unit // 2, t))
                    reduce_ring(unit, t).wait_send()

    def weight_sends(layer):
        for m in range(3):
            for k in (1, 2, 3):
                pre_copy(layer, m, k).wait_send()
            for p in range(4):
                for r in rounds(layer, m, p):
                    ring_copy(layer, r, m, p).wait_send()

    with jax.named_scope("barrier"):
        pl.semaphore_wait(barrier, len(peers))
    pre_start(0)
    run_layer(0, x_ref)
    for peer in token_peers:
        pl.semaphore_signal(ready, inc=1, device_id=peer, device_id_type=MESH_ID)
    weight_sends(0)
    run_layer(1, out_ref)
    weight_sends(1)


def moe_layers(ring_shape, stream, norm_w, router, routes, weights):
    tok_dev, d_model = stream.shape
    part = tok_dev // 4
    n_z, n_y, n_x = ring_shape
    vmem = pl.BlockSpec(memory_space=pltpu.VMEM)
    hbm = pl.BlockSpec(memory_space=pl.ANY)
    dma = pltpu.SemaphoreType.DMA
    n_exp, f_dev = weights[0].shape[1] // n_x, weights[0].shape[2]
    w_shape = (n_exp, 3, n_z, n_y, n_x, f_dev, d_model)
    return pl.pallas_call(
        functools.partial(kernel, ring_shape),
        name="moe_layers",
        out_shape=[jax.ShapeDtypeStruct(stream.shape, stream.dtype), jax.ShapeDtypeStruct(w_shape, jnp.bfloat16)],
        in_specs=[vmem] * 4 + [hbm] * 3,
        out_specs=[vmem, hbm],
        scratch_shapes=[
            pltpu.VMEM((UNITS, 2, 2, part, d_model), jnp.bfloat16),
            pltpu.VMEM((UNITS, 2, 2, router.shape[1], part), jnp.float32),
            pltpu.VMEM(w_shape, jnp.bfloat16),
            pltpu.VMEM((UNITS, 2, 2, part, d_model), jnp.float32),
            pltpu.VMEM((UNITS, 2, part, d_model), jnp.float32),
            pltpu.VMEM((12, part, d_model), jnp.float32),
            dma((2, 24)), dma((2, 24)), dma((2, 16)), dma((2, 16)), dma((2, 8)), dma((2, 8)), dma((2, 12)), dma((2, 12)),
            dma((6,)), dma((18,)), dma((18,)), dma((144,)), dma((144,)), dma((n_exp,)),
            pltpu.SemaphoreType.REGULAR,
        ],
        compiler_params=pltpu.CompilerParams(
            collective_id=0, has_side_effects=True, vmem_limit_bytes=67043328),
        cost_estimate=pl.CostEstimate(flops=104 * 10**9, bytes_accessed=64 * 2**20, transcendentals=0),
    )(stream, norm_w, router, routes, *weights)[0]


def solution(mesh):
    n_x = 4
    n_y = min(4, mesh.shape["fsdp"] // n_x)
    devices = mesh.devices.reshape(mesh.shape["rep"], mesh.shape["ep"], -1, n_y, n_x)
    cells = Mesh(devices, ("rep", "ep", "z", "y", "x"))
    ring_shape = devices.shape[2:]
    fsdp = ("z", "y", "x")
    token_spec = P(("rep", "ep") + fsdp, None)
    expert_in_spec = P(None, "ep", None, fsdp)
    expert_out_spec = P(None, "ep", fsdp, None)
    route_spec = P(None, ("rep", "ep") + fsdp, None)

    def device_step(x_in, norm_w, router_w, gate_w, up_w, down_w, routes):
        shards = (gate_w.transpose(0, 1, 3, 2), up_w.transpose(0, 1, 3, 2), down_w)
        return moe_layers(ring_shape, x_in, norm_w, router_w.transpose(0, 2, 1), routes.transpose(0, 2, 1), shards)

    return jax.shard_map(device_step, mesh=cells,
                         in_specs=(token_spec, P(), P(), expert_in_spec, expert_in_spec, expert_out_spec, route_spec),
                         out_specs=token_spec, check_vma=False)
```

```python
import functools

import jax
import jax.numpy as jnp
from jax import lax
from jax.experimental import pallas as pl
from jax.experimental.pallas import tpu as pltpu
from jax.sharding import Mesh, PartitionSpec as P

NORM_EPS = 1e-5
MESH_ID = pl.DeviceIdType.MESH

OWN, NEAR, FAR, MORE = range(4)
UNITS = 8
LATE_EVENTS = (
    ("own", 1, (2, 4)), ("rows", 1, (6, 9)), ("own", 2, (6, 8)),
    ("rest", 0, (11, 16)), ("rest", 1, (19, 27)), ("rest", 2, (32, 35)),
)


def kernel(ring_shape, x_ref, norm_ref, router_ref, routes_ref, gate_ref, up_ref, down_ref, out_ref, next_ref,
           h_all, g_all, w_v, acc, pair_in, ring_in,
           ag_send, ag_recv, agp_send, agp_recv, pair_send, pair_recv, ring_send, ring_recv,
           pre_own, pre_send, pre_recv, wr_send, wr_recv, w_sem, ready):
    part, d_model = h_all.shape[3], h_all.shape[4]
    n_exp = w_v.shape[0]
    n_z, n_y, n_x = ring_shape
    ep, x = lax.axis_index("ep"), lax.axis_index("x")
    z, y = lax.axis_index("z"), lax.axis_index("y")
    partner = {"ep": 1 - ep}
    owners = (x, lax.rem(x + y, 4))
    steps = UNITS * n_exp

    def remote(src, dst, send, recv, peer):
        return pltpu.make_async_remote_copy(src, dst, send, recv, device_id=peer, device_id_type=MESH_ID)

    def beside(layer, axis, stream):
        move = 1 + 2 * stream
        if layer == 0:
            return {"x": lax.rem(x + move, 4)}
        return {"x": lax.rem(x + axis * move, 4), "y": lax.rem(y + (1 - axis) * move, 4)}

    def next_row(layer, step):
        if layer == 0:
            return {"y": lax.rem(y + 4 + step, 4)}
        return {"x": lax.rem(x + 4 - step, 4), "y": lax.rem(y + 4 + step, 4)}

    token_peers = [beside(0, 0, 0), beside(0, 0, 1), beside(1, 0, 0), beside(1, 0, 1), partner]
    peers = token_peers + [{"x": lax.rem(x + 2, 4)}] + [next_row(1, step) for step in (1, -1)]
    if n_z > 1:
        peers += [{"z": lax.rem(z + 1, n_z)}, {"z": lax.rem(z + n_z - 1, n_z)}]
    barrier = pltpu.get_barrier_semaphore()
    for peer in peers:
        pl.semaphore_signal(barrier, inc=1, device_id=peer, device_id_type=MESH_ID)

    sources = (gate_ref, up_ref, down_ref)
    targets = (w_v, next_ref)

    def landing(layer, m):
        return targets[layer].at[:, m, z, 0 if layer else y, x]

    def pre_local(layer, m):
        return pltpu.make_async_copy(
            sources[m].at[layer, pl.ds(owners[layer] * n_exp, n_exp)], landing(layer, m),
            pre_own.at[layer * 3 + m])

    def pre_copy(layer, m, k):
        idx = (layer * 3 + m) * 3 + k - 1
        return remote(sources[m].at[layer, pl.ds(lax.rem(owners[layer] + k, 4) * n_exp, n_exp)],
                      landing(layer, m),
                      pre_send.at[idx], pre_recv.at[idx], {"x": lax.rem(x + k, 4)})

    def hops(along_z):
        return 3 if (n_z if along_z else n_y) > 1 else 0

    def ring_copy(r, m, p):
        step = 1 if p % 2 == 0 else -1
        along_z = (r < 3) == (p < 2)
        if r % 3 >= hops(along_z):
            return None
        pos = z if along_z else y
        i = lax.rem(pos + 4 - step * (r % 3), 4)
        if r < 3:
            piece = w_v.at[p, m, i, y] if along_z else w_v.at[p, m, z, i]
        else:
            piece = w_v.at[p, m, i] if along_z else w_v.at[p, m, :, i]
        idx = (r * 3 + m) * 4 + p
        peer = {"z": lax.rem(z + 4 + step, 4)} if along_z else next_row(0, step)
        return remote(piece, piece, wr_send.at[idx], wr_recv.at[idx], peer)

    def late_copy(stage, hop, m, p):
        if stage == "rows":
            step = 1 - hop % 2 * 2
            near, far = -step % 4, 2
            if hop < 2:
                src, dst = next_ref.at[p, m, z, 0], next_ref.at[p, m, z, near]
            else:
                xs = pl.ds(n_x // 2 * (hop - 2), n_x // 2)
                src, dst = next_ref.at[p, m, z, near, xs], next_ref.at[p, m, z, far, xs]
            peer = next_row(1, step)
        else:
            if hop >= hops(True):
                return None
            step = 1 - p % 2 * 2
            i = lax.rem(z + 4 - step * hop, 4)
            src = dst = next_ref.at[p, m, i, 0 if stage == "own" else pl.ds(1, n_y - 1)]
            peer = {"z": lax.rem(z + 4 + step, 4)}
        idx = 72 + (({"own": 0, "rows": 3, "rest": 7}[stage] + hop) * 3 + m) * 4 + p
        return remote(src, dst, wr_send.at[idx], wr_recv.at[idx], peer)

    def pre_start(layer):
        for m in range(3):
            for k in (1, 3, 2):
                pre_copy(layer, m, k).start()
            pre_local(layer, m).start()

    def pre_wait(layer, m):
        pre_local(layer, m).wait()
        for k in (1, 3, 2):
            pre_copy(layer, m, k).wait_recv()

    def then(before, after):
        if before is not None:
            before.wait_recv()
        if after is not None:
            after.start()

    def ring_event(r, m):
        with jax.named_scope(f"w0r{r}m{m}"):
            if r == 0:
                pre_wait(0, m)
            for p in range(4):
                last = [q for q in range(r) if ring_copy(q, m, p) is not None][-1:]
                after = ring_copy(r, m, p) if r < 6 else None
                if after is not None or r == 6:
                    then(ring_copy(last[0], m, p) if last else None, after)

    def ring_round(r):
        for m in range(3):
            ring_event(r, m)

    def late_event(stage, hop, pair):
        with jax.named_scope(f"w1{stage}{hop}p{pair}"):
            for p in (2 * pair, 2 * pair + 1):
                for m in range(3):
                    before = []
                    after = [late_copy(stage, hop, m, p)]
                    if stage == "rows":
                        before = [late_copy(stage, q, m, p) for q in range(2 * hop)]
                        after = [late_copy(stage, 2 * hop + q, m, p) for q in range(2)]
                    elif hop > 0:
                        before = [late_copy(stage, hop - 1, m, p)]
                    elif stage == "rest":
                        before = [late_copy("rows", q, m, p) for q in (2, 3)]
                    for copy in before:
                        then(copy, None)
                    for copy in after:
                        then(None, copy)

    def late_end(pair):
        with jax.named_scope(f"w1end{pair}"):
            for p in (2 * pair, 2 * pair + 1):
                for m in range(3):
                    then(late_copy("own", 2, m, p), None)
                    then(late_copy("rest", 2, m, p), None)

    loads = [pltpu.make_async_copy(next_ref.at[e], w_v.at[e], w_sem.at[e]) for e in range(n_exp)]

    def prepare(layer, stream_ref, axis):
        experts = router_ref.shape[1]
        for t in range(2):
            rows = pl.ds((2 * axis + t) * part, part)
            wide = stream_ref[rows, :].astype(jnp.float32)
            inv_rms = lax.rsqrt(jnp.mean(wide * wide, axis=-1, keepdims=True) + NORM_EPS)
            hidden = (wide * inv_rms * norm_ref[layer:layer + 1, :]).astype(jnp.bfloat16)
            h_all[axis, t, 0] = hidden
            logits = lax.dot_general(router_ref[layer], hidden, (((1,), (1,)), ((), ())),
                                     preferred_element_type=jnp.float32)
            ids = lax.broadcasted_iota(jnp.int32, (experts, part), 0)
            chosen = ids < 0
            for j in range(routes_ref.shape[1]):
                chosen |= routes_ref[layer, j:j + 1, (2 * axis + t) * part:(2 * axis + t + 1) * part] == ids
            top = jnp.max(jnp.where(chosen, logits, -jnp.inf), axis=0, keepdims=True)
            weight = jnp.where(chosen, jnp.exp(jnp.where(chosen, logits - top, 0.0)), 0.0)
            gates = weight / jnp.sum(weight, axis=0, keepdims=True)
            g_all[axis, t, 0] = jnp.where(chosen, gates, -1.0)

    def start(copies):
        for copy in copies:
            copy.start()

    def wait_recv(copies):
        for copy in copies:
            copy.wait_recv()

    def wait_send(copies):
        for copy in copies:
            copy.wait_send()

    def run_layer(layer, stream_ref, halfway=None):
        first = layer == 0
        group = ep * 4 + owners[layer]

        def pair_copy(unit):
            return (
                remote(h_all.at[unit, :, 0], h_all.at[unit, :, 1],
                       agp_send.at[layer, unit], agp_recv.at[layer, unit], partner),
                remote(g_all.at[unit, :, 0], g_all.at[unit, :, 1],
                       agp_send.at[layer, 8 + unit], agp_recv.at[layer, 8 + unit], partner),
            )

        def gather(axis, kind, t):
            src_kind, src_t, to = {
                (NEAR, 1): (OWN, 0, 0), (MORE, 1): (OWN, 1, 0), (FAR, 0): (NEAR, 1, 0),
                (NEAR, 0): (OWN, 1, 1), (MORE, 0): (OWN, 0, 1), (FAR, 1): (NEAR, 0, 1),
            }[kind, t]
            src, dst = 2 * src_kind + axis, 2 * kind + axis
            idx = 2 * (dst - 2) + t
            peer = beside(layer, axis, to)
            return (
                remote(h_all.at[src, src_t, 0], h_all.at[dst, t, 0],
                       ag_send.at[layer, idx], ag_recv.at[layer, idx], peer),
                remote(g_all.at[src, src_t, 0], g_all.at[dst, t, 0],
                       ag_send.at[layer, 12 + idx], ag_recv.at[layer, 12 + idx], peer),
            )

        def gather_start(axis):
            for t in range(2):
                start(gather(axis, NEAR, t))
            start(pair_copy(axis))
            for t in range(2):
                start(gather(axis, MORE, t))

        def arrive(kind, axis):
            with jax.named_scope(f"arr{kind}{axis}"):
                for t in range(2):
                    wait_recv(gather(axis, kind, t))
                    if kind == NEAR:
                        start(gather(axis, FAR, 1 - t))
                start(pair_copy(2 * kind + axis))

        def reduce_pair(unit):
            return remote(acc.at[unit, :, 1], pair_in.at[unit],
                          pair_send.at[layer, unit], pair_recv.at[layer, unit], partner)

        def place(unit, t):
            return 2 * (unit - 2) + t + 4 * layer * (unit // 6)

        def reduce_ring(unit, t):
            slot = 2 * (unit - 2) + t
            return remote(acc.at[unit, t, 0], ring_in.at[place(unit, t)], ring_send.at[layer, slot], ring_recv.at[layer, slot],
                          beside(layer, unit % 2, t))

        def add_pair(unit):
            with jax.named_scope("pairw"):
                reduce_pair(unit).wait_recv()
            acc[unit, :, 0] += pair_in[unit]

        def add_more(unit):
            with jax.named_scope("morew"):
                reduce_pair(unit).wait_recv()
                far = unit - 2 * (MORE - FAR)
                for t in range(2):
                    reduce_ring(far, t).wait_recv()
            for t in range(2):
                acc[unit, t, 0] += pair_in[unit, t] + ring_in[place(far, t)]

        def ring_start(unit):
            for t in range(2):
                reduce_ring(unit, t).start()

        plan = {}

        def at(t, action, *args):
            plan.setdefault(t, []).append((action, args))

        if first:
            for axis in range(2):
                prepare(layer, stream_ref, axis)
            for kind in (NEAR, MORE):
                for axis in range(2):
                    for t in range(2):
                        start(gather(axis, kind, t))
                    if kind == NEAR:
                        start(pair_copy(axis))
        else:
            prepare(layer, stream_ref, 0)
            with jax.named_scope("ready"):
                pl.semaphore_wait(ready, len(token_peers))
            gather_start(0)
        if first:
            for r in range(3):
                ring_round(r)
            arrive(NEAR, 0)
            arrive(NEAR, 1)
            pre_start(1)
            ring_round(3)
            ring_round(4)
            arrive(MORE, 0)
            arrive(MORE, 1)
            ring_round(5)
            arrive(FAR, 0)
            arrive(FAR, 1)
            ring_event(6, 0)
            ring_event(6, 1)
            for m in range(3):
                pre_wait(1, m)
            for pair in range(2):
                late_event("own", 0, pair)
            ring_event(6, 2)
            for pair in range(2):
                late_event("rows", 0, pair)
            for unit in range(UNITS):
                wait_recv(pair_copy(unit))
            for stage, hop, when in LATE_EVENTS:
                for pair in range(2):
                    at(when[pair], late_event, stage, hop, pair)
        else:
            halfway()
            prepare(layer, stream_ref, 1)
            gather_start(1)
            late_end(0)
            start(loads[:2])
            at(0, loads[0].wait)
            at(1, loads[1].wait)
            at(1, late_end, 1)
            at(1, start, loads[2:])
            at(2, loads[2].wait)
            at(3, loads[3].wait)

            for axis in range(2):
                at(3, arrive, NEAR, axis)
                at(6, arrive, MORE, axis)
                at(9, arrive, FAR, axis)

        def unit_of(k):
            if first:
                return jnp.where(k < 2, k + 2 * FAR, jnp.where(k < 4, k, jnp.where(k < 6, k + 2, k - 6)))
            return jnp.where(k == 0, 0, jnp.where(k == UNITS - 1, 1, k + 1))

        def step_fn(step, carry):
            k, e = step // n_exp, step % n_exp
            before, late = unit_of(k - 1), unit_of(k - 2)
            kind, late_kind = before // 2, late // 2

            def planned(e_static):
                for t in sorted(plan):
                    if t < steps and t % n_exp == e_static:
                        @pl.when(k == t // n_exp)
                        def _():
                            for action, args in plan[t]:
                                action(*args)

            @pl.when(e == 0)
            def _():
                planned(0)

                @pl.when(k >= 1)
                def _():
                    reduce_pair(before).start()

                if not first:
                    wait_recv(pair_copy(unit_of(k)))

            def sums(mask):
                @pl.when(mask & (k >= 1) & (kind != MORE))
                def _():
                    add_pair(before)

                @pl.when(mask & ((k >= 2) & (late_kind == MORE) if first else (k >= 1) & (kind == MORE)))
                def _():
                    add_more(late if first else before)

            def leave(mask):
                @pl.when(mask & (k >= 1) & (kind != OWN) & ((kind != MORE) if first else True))
                def _():
                    ring_start(before)

                if first:
                    @pl.when(mask & (k >= 2) & (late_kind == MORE))
                    def _():
                        ring_start(late)

            hurry = k == 1 if first else (k == 4) | (k == 5) | (k == UNITS - 1)

            @pl.when(e == 1)
            def _():
                planned(1)
                sums(hurry)

            @pl.when(e == 2)
            def _():
                planned(2)
                sums(jnp.logical_not(hurry))
                leave(hurry)

            @pl.when(e == 3)
            def _():
                planned(3)
                leave(jnp.logical_not(hurry))

            unit = unit_of(k)
            with jax.named_scope("load"):
                tokens = h_all[unit].reshape(-1, d_model)
            gate_w = w_v[e, 0].reshape(-1, d_model)
            up_w = w_v[e, 1].reshape(-1, d_model)
            down_w = w_v[e, 2].reshape(-1, d_model)
            d_ff = gate_w.shape[0]
            inner = []
            for f in range(0, d_ff, 256):
                nt = (((1,), (1,)), ((), ()))
                u = lax.dot_general(tokens, gate_w[f:f + 256], nt, preferred_element_type=jnp.float32)
                v = lax.dot_general(tokens, up_w[f:f + 256], nt, preferred_element_type=jnp.float32)
                inner.append((jax.nn.silu(u) * v).astype(jnp.bfloat16))
            inner = jnp.concatenate(inner, axis=1)
            row = group * n_exp + e
            gate_cols = []
            for t in range(2):
                for s in range(2):
                    gates = g_all[unit, t, s, pl.ds(row, 1), :]
                    gate_cols.append(jnp.broadcast_to(gates, (128, part)).T)
            gate_b = jnp.concatenate(gate_cols, axis=0)
            gate_b = jnp.concatenate([gate_b, gate_b], axis=1)
            start_sum = e == 0
            for c in range(0, d_model, 256):
                o = jnp.dot(inner, down_w[:, c:c + 256], preferred_element_type=jnp.float32)
                o = o.astype(jnp.bfloat16).astype(jnp.float32)
                new = jnp.where(gate_b >= 0.0, gate_b * o, 0.0).reshape(2, 2, part, 256)
                prev = jnp.where(start_sum, 0.0, acc[unit, :, :, :, c:c + 256])
                acc[unit, :, :, :, c:c + 256] = prev + new
            return carry

        lax.fori_loop(0, steps, step_fn, 0)
        reduce_pair(1).start()
        for t in sorted(plan):
            if t >= steps:
                for action, args in plan[t]:
                    action(*args)
        add_pair(1)

        def end_near(axis):
            near = 2 * NEAR + axis
            for t in range(2):
                with jax.named_scope("fin1"):
                    reduce_ring(near, 1 - t).wait_recv()
                rows = pl.ds((2 * axis + t) * part, part)
                acc[axis, t, 0] += stream_ref[rows, :].astype(jnp.float32) + ring_in[place(near, 1 - t)]

        def end_more(axis):
            more = 2 * MORE + axis
            for t in range(2):
                with jax.named_scope("fin2"):
                    reduce_ring(more, t).wait_recv()
                rows = pl.ds((2 * axis + t) * part, part)
                out_ref[rows, :] = (acc[axis, t, 0] + ring_in[place(more, t)]).astype(out_ref.dtype)

        def end_sends():
            for axis in range(2):
                for t in range(2):
                    reduce_ring(2 * MORE + axis, t).wait_send()

        end_near(0)
        end_near(1)
        for unit in range(UNITS):
            wait_send(pair_copy(unit))
            reduce_pair(unit).wait_send()
            if unit >= 2:
                for t in range(2):
                    wait_send(gather(unit % 2, unit // 2, t))
                    if unit < 2 * MORE:
                        reduce_ring(unit, t).wait_send()
        return end_more, end_sends

    def weight_sends(layer):
        for m in range(3):
            for k in (1, 2, 3):
                pre_copy(layer, m, k).wait_send()
            for p in range(4):
                if layer == 0:
                    copies = [ring_copy(r, m, p) for r in range(6)]
                else:
                    copies = [late_copy(stage, hop, m, p) for stage in ("own", "rest") for hop in range(3)]
                    copies += [late_copy("rows", hop, m, p) for hop in range(4)]
                wait_send([copy for copy in copies if copy is not None])

    with jax.named_scope("barrier"):
        pl.semaphore_wait(barrier, len(peers))
    pre_start(0)
    end_more, end_sends = run_layer(0, x_ref)
    weight_sends(0)
    for peer in token_peers:
        pl.semaphore_signal(ready, inc=1, device_id=peer, device_id_type=MESH_ID)
    end_more(0)

    def halfway():
        end_more(1)
        end_sends()

    end_more_1, end_sends_1 = run_layer(1, out_ref, halfway)
    end_more_1(0)
    end_more_1(1)
    end_sends_1()
    weight_sends(1)


def moe_layers(ring_shape, stream, norm_w, router, routes, weights):
    tok_dev, d_model = stream.shape
    part = tok_dev // 4
    n_z, n_y, n_x = ring_shape
    vmem = pl.BlockSpec(memory_space=pltpu.VMEM)
    hbm = pl.BlockSpec(memory_space=pl.ANY)
    dma = pltpu.SemaphoreType.DMA
    n_exp, f_dev = weights[0].shape[1] // n_x, weights[0].shape[2]
    w_shape = (n_exp, 3, n_z, n_y, n_x, f_dev, d_model)
    return pl.pallas_call(
        functools.partial(kernel, ring_shape),
        name="moe_layers",
        out_shape=[jax.ShapeDtypeStruct(stream.shape, stream.dtype), jax.ShapeDtypeStruct(w_shape, jnp.bfloat16)],
        in_specs=[vmem] * 4 + [hbm] * 3,
        out_specs=[vmem, hbm],
        scratch_shapes=[
            pltpu.VMEM((UNITS, 2, 2, part, d_model), jnp.bfloat16),
            pltpu.VMEM((UNITS, 2, 2, router.shape[1], part), jnp.float32),
            pltpu.VMEM(w_shape, jnp.bfloat16),
            pltpu.VMEM((UNITS, 2, 2, part, d_model), jnp.float32),
            pltpu.VMEM((UNITS, 2, part, d_model), jnp.float32),
            pltpu.VMEM((16, part, d_model), jnp.float32),
            dma((2, 24)), dma((2, 24)), dma((2, 16)), dma((2, 16)), dma((2, 8)), dma((2, 8)), dma((2, 12)), dma((2, 12)),
            dma((6,)), dma((18,)), dma((18,)), dma((192,)), dma((192,)), dma((n_exp,)),
            pltpu.SemaphoreType.REGULAR,
        ],
        compiler_params=pltpu.CompilerParams(
            collective_id=0, has_side_effects=True, vmem_limit_bytes=67043328),
        cost_estimate=pl.CostEstimate(flops=104 * 10**9, bytes_accessed=64 * 2**20, transcendentals=0),
    )(stream, norm_w, router, routes, *weights)[0]


def solution(mesh):
    n_x = 4
    n_y = min(4, mesh.shape["fsdp"] // n_x)
    devices = mesh.devices.reshape(mesh.shape["rep"], mesh.shape["ep"], -1, n_y, n_x)
    cells = Mesh(devices, ("rep", "ep", "z", "y", "x"))
    ring_shape = devices.shape[2:]
    fsdp = ("z", "y", "x")
    token_spec = P(("rep", "ep") + fsdp, None)
    expert_in_spec = P(None, "ep", None, fsdp)
    expert_out_spec = P(None, "ep", fsdp, None)
    route_spec = P(None, ("rep", "ep") + fsdp, None)

    def device_step(x_in, norm_w, router_w, gate_w, up_w, down_w, routes):
        shards = (gate_w.transpose(0, 1, 3, 2), up_w.transpose(0, 1, 3, 2), down_w)
        return moe_layers(ring_shape, x_in, norm_w, router_w.transpose(0, 2, 1), routes.transpose(0, 2, 1), shards)

    return jax.shard_map(device_step, mesh=cells,
                         in_specs=(token_spec, P(), P(), expert_in_spec, expert_in_spec, expert_out_spec, route_spec),
                         out_specs=token_spec, check_vma=False)
```

```python
import functools

import jax
import jax.numpy as jnp
from jax import lax
from jax.experimental import pallas as pl
from jax.experimental.pallas import tpu as pltpu
from jax.sharding import Mesh, PartitionSpec as P

NORM_EPS = 1e-5
MESH_ID = pl.DeviceIdType.MESH

OWN, NEAR, FAR, MORE = range(4)
UNITS = 8
LATE_EVENTS = (
    ("own", 1, (2, 4)), ("rows", 1, (6, 9)), ("own", 2, (6, 8)),
    ("rest", 0, (11, 16)), ("rest", 1, (19, 27)), ("rest", 2, (32, 35)),
)


def kernel(ring_shape, x_ref, norm_ref, router_ref, routes_ref, gate_ref, up_ref, down_ref, out_ref, next_ref,
           h_all, g_all, w_v, acc, pair_in, ring_in,
           ag_send, ag_recv, agp_send, agp_recv, pair_send, pair_recv, ring_send, ring_recv,
           pre_own, pre_send, pre_recv, wr_send, wr_recv, w_sem, ready):
    part, d_model = h_all.shape[3], h_all.shape[4]
    n_exp = w_v.shape[0]
    n_z, n_y, n_x = ring_shape
    ep, x = lax.axis_index("ep"), lax.axis_index("x")
    z, y = lax.axis_index("z"), lax.axis_index("y")
    partner = {"ep": 1 - ep}
    owners = (x, lax.rem(x + y, 4))
    steps = UNITS * n_exp

    def remote(src, dst, send, recv, peer):
        return pltpu.make_async_remote_copy(src, dst, send, recv, device_id=peer, device_id_type=MESH_ID)

    def beside(layer, axis, stream):
        move = 1 + 2 * stream
        if layer == 0:
            return {"x": lax.rem(x + move, 4)}
        return {"x": lax.rem(x + axis * move, 4), "y": lax.rem(y + (1 - axis) * move, 4)}

    def next_row(layer, step):
        if layer == 0:
            return {"y": lax.rem(y + 4 + step, 4)}
        return {"x": lax.rem(x + 4 - step, 4), "y": lax.rem(y + 4 + step, 4)}

    token_peers = [beside(0, 0, 0), beside(0, 0, 1), beside(1, 0, 0), beside(1, 0, 1), partner]
    peers = token_peers + [{"x": lax.rem(x + 2, 4)}] + [next_row(1, step) for step in (1, -1)]
    if n_z > 1:
        peers += [{"z": lax.rem(z + 1, n_z)}, {"z": lax.rem(z + n_z - 1, n_z)}]
    barrier = pltpu.get_barrier_semaphore()
    for peer in peers:
        pl.semaphore_signal(barrier, inc=1, device_id=peer, device_id_type=MESH_ID)

    sources = (gate_ref, up_ref, down_ref)
    targets = (w_v, next_ref)

    def landing(layer, m):
        return targets[layer].at[:, m, z, 0 if layer else y, x]

    def pre_local(layer, m):
        return pltpu.make_async_copy(
            sources[m].at[layer, pl.ds(owners[layer] * n_exp, n_exp)], landing(layer, m),
            pre_own.at[layer * 3 + m])

    def pre_copy(layer, m, k):
        idx = (layer * 3 + m) * 3 + k - 1
        return remote(sources[m].at[layer, pl.ds(lax.rem(owners[layer] + k, 4) * n_exp, n_exp)],
                      landing(layer, m),
                      pre_send.at[idx], pre_recv.at[idx], {"x": lax.rem(x + k, 4)})

    def hops(along_z):
        return 3 if (n_z if along_z else n_y) > 1 else 0

    def ring_copy(r, m, p):
        step = 1 if p % 2 == 0 else -1
        along_z = (r < 3) == (p < 2)
        if r % 3 >= hops(along_z):
            return None
        pos = z if along_z else y
        i = lax.rem(pos + 4 - step * (r % 3), 4)
        if r < 3:
            piece = w_v.at[p, m, i, y] if along_z else w_v.at[p, m, z, i]
        else:
            piece = w_v.at[p, m, i] if along_z else w_v.at[p, m, :, i]
        idx = (r * 3 + m) * 4 + p
        peer = {"z": lax.rem(z + 4 + step, 4)} if along_z else next_row(0, step)
        return remote(piece, piece, wr_send.at[idx], wr_recv.at[idx], peer)

    def late_copy(stage, hop, p):
        if stage == "rows":
            step = 1 - hop % 2 * 2
            near, far = -step % 4, 2
            if hop < 2:
                src, dst = next_ref.at[p, :, z, 0], next_ref.at[p, :, z, near]
            else:
                xs = pl.ds(n_x // 2 * (hop - 2), n_x // 2)
                src, dst = next_ref.at[p, :, z, near, xs], next_ref.at[p, :, z, far, xs]
            peer = next_row(1, step)
        else:
            if hop >= hops(True):
                return None
            step = 1 - p % 2 * 2
            i = lax.rem(z + 4 - step * hop, 4)
            src = dst = next_ref.at[p, :, i, 0 if stage == "own" else pl.ds(1, n_y - 1)]
            peer = {"z": lax.rem(z + 4 + step, 4)}
        idx = 72 + ({"own": 0, "rows": 3, "rest": 7}[stage] + hop) * 4 + p
        return remote(src, dst, wr_send.at[idx], wr_recv.at[idx], peer)

    def pre_start(layer):
        for m in range(3):
            for k in (1, 3, 2):
                pre_copy(layer, m, k).start()
            pre_local(layer, m).start()

    def pre_wait(layer, m):
        pre_local(layer, m).wait()
        for k in (1, 3, 2):
            pre_copy(layer, m, k).wait_recv()

    def then(before, after):
        if before is not None:
            before.wait_recv()
        if after is not None:
            after.start()

    def ring_event(r, m):
        with jax.named_scope(f"w0r{r}m{m}"):
            if r == 0:
                pre_wait(0, m)
            for p in range(4):
                last = [q for q in range(r) if ring_copy(q, m, p) is not None][-1:]
                after = ring_copy(r, m, p) if r < 6 else None
                if after is not None or r == 6:
                    then(ring_copy(last[0], m, p) if last else None, after)

    def ring_round(r):
        for m in range(3):
            ring_event(r, m)

    def late_event(stage, hop, pair):
        with jax.named_scope(f"w1{stage}{hop}p{pair}"):
            for p in (2 * pair, 2 * pair + 1):
                before = []
                after = [late_copy(stage, hop, p)]
                if stage == "rows":
                    before = [late_copy(stage, q, p) for q in range(2 * hop)]
                    after = [late_copy(stage, 2 * hop + q, p) for q in range(2)]
                elif hop > 0:
                    before = [late_copy(stage, hop - 1, p)]
                elif stage == "rest":
                    before = [late_copy("rows", q, p) for q in (2, 3)]
                for copy in before:
                    then(copy, None)
                for copy in after:
                    then(None, copy)

    def late_end(pair):
        with jax.named_scope(f"w1end{pair}"):
            for p in (2 * pair, 2 * pair + 1):
                then(late_copy("own", 2, p), None)
                then(late_copy("rest", 2, p), None)

    loads = [pltpu.make_async_copy(next_ref.at[e], w_v.at[e], w_sem.at[e]) for e in range(n_exp)]

    def prepare(layer, stream_ref, axis):
        experts = router_ref.shape[1]
        for t in range(2):
            rows = pl.ds((2 * axis + t) * part, part)
            wide = stream_ref[rows, :].astype(jnp.float32)
            inv_rms = lax.rsqrt(jnp.mean(wide * wide, axis=-1, keepdims=True) + NORM_EPS)
            hidden = (wide * inv_rms * norm_ref[layer:layer + 1, :]).astype(jnp.bfloat16)
            h_all[axis, t, 0] = hidden
            logits = lax.dot_general(router_ref[layer], hidden, (((1,), (1,)), ((), ())),
                                     preferred_element_type=jnp.float32)
            ids = lax.broadcasted_iota(jnp.int32, (experts, part), 0)
            chosen = ids < 0
            for j in range(routes_ref.shape[1]):
                chosen |= routes_ref[layer, j:j + 1, (2 * axis + t) * part:(2 * axis + t + 1) * part] == ids
            top = jnp.max(jnp.where(chosen, logits, -jnp.inf), axis=0, keepdims=True)
            weight = jnp.where(chosen, jnp.exp(jnp.where(chosen, logits - top, 0.0)), 0.0)
            gates = weight / jnp.sum(weight, axis=0, keepdims=True)
            g_all[axis, t, 0] = jnp.where(chosen, gates, -1.0)

    def start(copies):
        for copy in copies:
            copy.start()

    def wait_recv(copies):
        for copy in copies:
            copy.wait_recv()

    def wait_send(copies):
        for copy in copies:
            copy.wait_send()

    def early_sends():
        for m in range(3):
            for k in (1, 2, 3):
                pre_copy(0, m, k).wait_send()
            for p in range(4):
                wait_send([copy for copy in (ring_copy(r, m, p) for r in range(6)) if copy is not None])

    def late_sends(last):
        for p in range(4):
            copies = [late_copy("rest", 2, p)]
            if not last:
                copies = [late_copy(stage, hop, p) for stage in ("own", "rest") for hop in range(3)][:5]
                copies += [late_copy("rows", hop, p) for hop in range(4)]
            wait_send([copy for copy in copies if copy is not None])
        if not last:
            for m in range(3):
                for k in (1, 2, 3):
                    pre_copy(1, m, k).wait_send()

    def by_rows(update):
        chunk = min(32, part)

        def body(i, carry):
            update(pl.ds(pl.multiple_of(i * chunk, chunk), chunk), i * chunk, chunk)
            return carry

        lax.fori_loop(0, part // chunk, body, 0)

    def run_layer(layer, stream_ref, halfway=None):
        first = layer == 0
        group = ep * 4 + owners[layer]

        def pair_copy(unit):
            return (
                remote(h_all.at[unit, :, 0], h_all.at[unit, :, 1],
                       agp_send.at[unit], agp_recv.at[unit], partner),
                remote(g_all.at[unit, :, 0], g_all.at[unit, :, 1],
                       agp_send.at[8 + unit], agp_recv.at[8 + unit], partner),
            )

        def gather(axis, kind, t):
            src_kind, src_t, to = {
                (NEAR, 1): (OWN, 0, 0), (MORE, 1): (OWN, 1, 0), (FAR, 0): (NEAR, 1, 0),
                (NEAR, 0): (OWN, 1, 1), (MORE, 0): (OWN, 0, 1), (FAR, 1): (NEAR, 0, 1),
            }[kind, t]
            src, dst = 2 * src_kind + axis, 2 * kind + axis
            idx = 2 * (dst - 2) + t
            peer = beside(layer, axis, to)
            return (
                remote(h_all.at[src, src_t, 0], h_all.at[dst, t, 0],
                       ag_send.at[idx], ag_recv.at[idx], peer),
                remote(g_all.at[src, src_t, 0], g_all.at[dst, t, 0],
                       ag_send.at[12 + idx], ag_recv.at[12 + idx], peer),
            )

        def gather_start(axis):
            for t in range(2):
                start(gather(axis, NEAR, t))
            start(pair_copy(axis))
            for t in range(2):
                start(gather(axis, MORE, t))

        def arrive(kind, axis):
            with jax.named_scope(f"arr{kind}{axis}"):
                for t in range(2):
                    wait_recv(gather(axis, kind, t))
                    if kind == NEAR:
                        start(gather(axis, FAR, 1 - t))
                start(pair_copy(2 * kind + axis))

        def reduce_pair(unit):
            return remote(acc.at[unit, :, 1], pair_in.at[unit],
                          pair_send.at[unit], pair_recv.at[unit], partner)

        def place(unit, t):
            return 2 * (unit - 2) + t + 4 * layer * (unit // 6)

        def reduce_ring(unit, t):
            slot = 2 * (unit - 2) + t
            return remote(acc.at[unit, t, 0], ring_in.at[place(unit, t)], ring_send.at[layer, slot], ring_recv.at[layer, slot],
                          beside(layer, unit % 2, t))

        def add_pair(unit):
            with jax.named_scope("pairw"):
                reduce_pair(unit).wait_recv()

            def update(rows, first_row, n):
                for t in range(2):
                    acc[unit, t, 0, rows] += pair_in[unit, t, rows]

            by_rows(update)

        def add_more(unit):
            with jax.named_scope("morew"):
                reduce_pair(unit).wait_recv()
                far = unit - 2 * (MORE - FAR)
                for t in range(2):
                    reduce_ring(far, t).wait_recv()

            def update(rows, first_row, n):
                for t in range(2):
                    acc[unit, t, 0, rows] += pair_in[unit, t, rows] + ring_in[place(far, t), rows]

            by_rows(update)

        def ring_start(unit):
            for t in range(2):
                reduce_ring(unit, t).start()

        plan = {}

        def at(t, action, *args):
            plan.setdefault(t, []).append((action, args))

        if first:
            for axis in range(2):
                prepare(layer, stream_ref, axis)
            for kind in (NEAR, MORE):
                for axis in range(2):
                    for t in range(2):
                        start(gather(axis, kind, t))
                    if kind == NEAR:
                        start(pair_copy(axis))
        else:
            prepare(layer, stream_ref, 0)
            with jax.named_scope("ready"):
                pl.semaphore_wait(ready, len(token_peers))
            gather_start(0)
        if first:
            for r in range(3):
                ring_round(r)
            arrive(NEAR, 0)
            arrive(NEAR, 1)
            pre_start(1)
            ring_round(3)
            ring_round(4)
            arrive(MORE, 0)
            arrive(MORE, 1)
            ring_round(5)
            arrive(FAR, 0)
            arrive(FAR, 1)
            ring_event(6, 0)
            ring_event(6, 1)
            for m in range(3):
                pre_wait(1, m)
            for pair in range(2):
                late_event("own", 0, pair)
            ring_event(6, 2)
            for pair in range(2):
                late_event("rows", 0, pair)
            for unit in range(UNITS):
                wait_recv(pair_copy(unit))
            for stage, hop, when in LATE_EVENTS:
                for pair in range(2):
                    at(when[pair], late_event, stage, hop, pair)
        else:
            halfway()
            prepare(layer, stream_ref, 1)
            gather_start(1)
            late_end(0)
            start(loads[:2])
            late_sends(last=False)
            for axis in range(2):
                arrive(NEAR, axis)
            late_end(1)
            start(loads[2:])
            for e in range(n_exp):
                at(e, loads[e].wait)
            for axis in range(2):
                at(3, arrive, MORE, axis)
                at(5, arrive, FAR, axis)

        def unit_of(k):
            if first:
                return jnp.where(k < 2, k + 2 * FAR, jnp.where(k < 4, k, jnp.where(k < 6, k + 2, k - 6)))
            return jnp.where(k < 6, k + 2, k - 6)

        def step_fn(step, carry):
            k, e = step // n_exp, step % n_exp
            before, late = unit_of(k - 1), unit_of(k - 2)
            kind, late_kind = before // 2, late // 2

            def planned(e_static):
                for t in sorted(plan):
                    if t < steps and t % n_exp == e_static:
                        @pl.when(k == t // n_exp)
                        def _():
                            for action, args in plan[t]:
                                action(*args)

            @pl.when(e == 0)
            def _():
                planned(0)

                @pl.when(k >= 1)
                def _():
                    reduce_pair(before).start()

                if not first:
                    wait_recv(pair_copy(unit_of(k)))

            def sums(mask):
                @pl.when(mask & (k >= 1) & (kind != MORE))
                def _():
                    add_pair(before)

                @pl.when(mask & ((k >= 2) & (late_kind == MORE) if first else (k >= 1) & (kind == MORE)))
                def _():
                    add_more(late if first else before)

            def leave(mask):
                @pl.when(mask & (k >= 1) & (kind != OWN) & ((kind != MORE) if first else True))
                def _():
                    ring_start(before)

                if first:
                    @pl.when(mask & (k >= 2) & (late_kind == MORE))
                    def _():
                        ring_start(late)

            hurry = k == 1 if first else (k == 4) | (k == 6)

            @pl.when(e == 1)
            def _():
                planned(1)
                sums(hurry)

            @pl.when(e == 2)
            def _():
                planned(2)
                sums(jnp.logical_not(hurry))
                leave(hurry)

            @pl.when(e == 3)
            def _():
                planned(3)
                leave(jnp.logical_not(hurry))

            unit = unit_of(k)
            with jax.named_scope("load"):
                tokens = h_all[unit].reshape(-1, d_model)
            gate_w = w_v[e, 0].reshape(-1, d_model)
            up_w = w_v[e, 1].reshape(-1, d_model)
            down_w = w_v[e, 2].reshape(-1, d_model)
            d_ff = gate_w.shape[0]
            inner = []
            for f in range(0, d_ff, 256):
                nt = (((1,), (1,)), ((), ()))
                u = lax.dot_general(tokens, gate_w[f:f + 256], nt, preferred_element_type=jnp.float32)
                v = lax.dot_general(tokens, up_w[f:f + 256], nt, preferred_element_type=jnp.float32)
                inner.append((jax.nn.silu(u) * v).astype(jnp.bfloat16))
            inner = jnp.concatenate(inner, axis=1)
            row = group * n_exp + e
            gate_cols = []
            for t in range(2):
                for s in range(2):
                    gates = g_all[unit, t, s, pl.ds(row, 1), :]
                    gate_cols.append(jnp.broadcast_to(gates, (128, part)).T)
            gate_b = jnp.concatenate(gate_cols, axis=0)
            gate_b = jnp.concatenate([gate_b, gate_b], axis=1)
            start_sum = e == 0
            for c in range(0, d_model, 256):
                o = jnp.dot(inner, down_w[:, c:c + 256], preferred_element_type=jnp.float32)
                o = o.astype(jnp.bfloat16).astype(jnp.float32)
                new = jnp.where(gate_b >= 0.0, gate_b * o, 0.0).reshape(2, 2, part, 256)
                prev = jnp.where(start_sum, 0.0, acc[unit, :, :, :, c:c + 256])
                acc[unit, :, :, :, c:c + 256] = prev + new
            return carry

        lax.fori_loop(0, steps, step_fn, 0)
        reduce_pair(1).start()
        for t in sorted(plan):
            if t >= steps:
                for action, args in plan[t]:
                    action(*args)

        def end_near(axis):
            near = 2 * NEAR + axis
            for t in range(2):
                with jax.named_scope("fin1"):
                    reduce_ring(near, 1 - t).wait_recv()

                def update(rows, first_row, n):
                    own = pl.ds(pl.multiple_of((2 * axis + t) * part + first_row, n), n)
                    acc[axis, t, 0, rows] += stream_ref[own, :].astype(jnp.float32) + ring_in[place(near, 1 - t), rows]

                by_rows(update)

        def end_more(axis):
            more = 2 * MORE + axis
            for t in range(2):
                with jax.named_scope("fin2"):
                    reduce_ring(more, t).wait_recv()

                def update(rows, first_row, n):
                    own = pl.ds(pl.multiple_of((2 * axis + t) * part + first_row, n), n)
                    out_ref[own, :] = (acc[axis, t, 0, rows] + ring_in[place(more, t), rows]).astype(out_ref.dtype)

                by_rows(update)

        def end_sends():
            for axis in range(2):
                for t in range(2):
                    reduce_ring(2 * MORE + axis, t).wait_send()

        end_near(0)
        if not first:
            end_more(0)
        add_pair(1)
        end_near(1)
        for unit in range(UNITS):
            wait_send(pair_copy(unit))
            reduce_pair(unit).wait_send()
            if unit >= 2:
                for t in range(2):
                    wait_send(gather(unit % 2, unit // 2, t))
                    if unit < 2 * MORE:
                        reduce_ring(unit, t).wait_send()
        return end_more, end_sends

    with jax.named_scope("barrier"):
        pl.semaphore_wait(barrier, len(peers))
    pre_start(0)
    end_more, end_sends = run_layer(0, x_ref)
    early_sends()
    for peer in token_peers:
        pl.semaphore_signal(ready, inc=1, device_id=peer, device_id_type=MESH_ID)
    end_more(0)

    def halfway():
        end_more(1)
        end_sends()

    end_more_1, end_sends_1 = run_layer(1, out_ref, halfway)
    end_more_1(1)
    end_sends_1()
    late_sends(last=True)


def moe_layers(ring_shape, stream, norm_w, router, routes, weights):
    tok_dev, d_model = stream.shape
    part = tok_dev // 4
    n_z, n_y, n_x = ring_shape
    vmem = pl.BlockSpec(memory_space=pltpu.VMEM)
    hbm = pl.BlockSpec(memory_space=pl.ANY)
    dma = pltpu.SemaphoreType.DMA
    n_exp, f_dev = weights[0].shape[1] // n_x, weights[0].shape[2]
    w_shape = (n_exp, 3, n_z, n_y, n_x, f_dev, d_model)
    return pl.pallas_call(
        functools.partial(kernel, ring_shape),
        name="moe_layers",
        out_shape=[jax.ShapeDtypeStruct(stream.shape, stream.dtype), jax.ShapeDtypeStruct(w_shape, jnp.bfloat16)],
        in_specs=[vmem] * 4 + [hbm] * 3,
        out_specs=[vmem, hbm],
        scratch_shapes=[
            pltpu.VMEM((UNITS, 2, 2, part, d_model), jnp.bfloat16),
            pltpu.VMEM((UNITS, 2, 2, router.shape[1], part), jnp.float32),
            pltpu.VMEM(w_shape, jnp.bfloat16),
            pltpu.VMEM((UNITS, 2, 2, part, d_model), jnp.float32),
            pltpu.VMEM((UNITS, 2, part, d_model), jnp.float32),
            pltpu.VMEM((16, part, d_model), jnp.float32),
            dma((24,)), dma((24,)), dma((16,)), dma((16,)), dma((8,)), dma((8,)), dma((2, 12)), dma((2, 12)),
            dma((6,)), dma((18,)), dma((18,)), dma((112,)), dma((112,)), dma((n_exp,)),
            pltpu.SemaphoreType.REGULAR,
        ],
        compiler_params=pltpu.CompilerParams(
            collective_id=0, has_side_effects=True, vmem_limit_bytes=67043328),
        cost_estimate=pl.CostEstimate(flops=104 * 10**9, bytes_accessed=64 * 2**20, transcendentals=0),
    )(stream, norm_w, router, routes, *weights)[0]


def solution(mesh):
    n_x = 4
    n_y = min(4, mesh.shape["fsdp"] // n_x)
    devices = mesh.devices.reshape(mesh.shape["rep"], mesh.shape["ep"], -1, n_y, n_x)
    cells = Mesh(devices, ("rep", "ep", "z", "y", "x"))
    ring_shape = devices.shape[2:]
    fsdp = ("z", "y", "x")
    token_spec = P(("rep", "ep") + fsdp, None)
    expert_in_spec = P(None, "ep", None, fsdp)
    expert_out_spec = P(None, "ep", fsdp, None)
    route_spec = P(None, ("rep", "ep") + fsdp, None)

    def device_step(x_in, norm_w, router_w, gate_w, up_w, down_w, routes):
        shards = (gate_w.transpose(0, 1, 3, 2), up_w.transpose(0, 1, 3, 2), down_w)
        return moe_layers(ring_shape, x_in, norm_w, router_w.transpose(0, 2, 1), routes.transpose(0, 2, 1), shards)

    return jax.shard_map(device_step, mesh=cells,
                         in_specs=(token_spec, P(), P(), expert_in_spec, expert_in_spec, expert_out_spec, route_spec),
                         out_specs=token_spec, check_vma=False)
```

```python
import functools

import jax
import jax.numpy as jnp
from jax import lax
from jax.experimental import pallas as pl
from jax.experimental.pallas import tpu as pltpu
from jax.sharding import Mesh, PartitionSpec as P

NORM_EPS = 1e-5
MESH_ID = pl.DeviceIdType.MESH

OWN, NEAR, FAR, MORE = range(4)
UNITS = 8
LATE_EVENTS = (
    ("own", 1, (2, 4)), ("rows", 1, (6, 9)), ("own", 2, (6, 8)),
    ("rest", 0, (11, 16)), ("rest", 1, (19, 27)), ("rest", 2, (32, 35)),
)


def kernel(ring_shape, x_ref, norm_ref, router_ref, routes_ref, gate_ref, up_ref, down_ref, out_ref, next_ref,
           h_all, g_all, w_v, acc, pair_in, ring_in,
           ag_send, ag_recv, agp_send, agp_recv, pair_send, pair_recv, ring_send, ring_recv,
           pre_own, pre_send, pre_recv, wr_send, wr_recv, w_sem, ready):
    part, d_model = h_all.shape[3], h_all.shape[4]
    n_exp = w_v.shape[0]
    n_z, n_y, n_x = ring_shape
    ep, x = lax.axis_index("ep"), lax.axis_index("x")
    z, y = lax.axis_index("z"), lax.axis_index("y")
    partner = {"ep": 1 - ep}
    owners = (x, lax.rem(x + y, 4))
    steps = UNITS * n_exp

    def remote(src, dst, send, recv, peer):
        return pltpu.make_async_remote_copy(src, dst, send, recv, device_id=peer, device_id_type=MESH_ID)

    def beside(layer, axis, stream):
        move = 1 + 2 * stream
        if layer == 0:
            return {"x": lax.rem(x + move, 4)}
        return {"x": lax.rem(x + axis * move, 4), "y": lax.rem(y + (1 - axis) * move, 4)}

    def next_row(layer, step):
        if layer == 0:
            return {"y": lax.rem(y + 4 + step, 4)}
        return {"x": lax.rem(x + 4 - step, 4), "y": lax.rem(y + 4 + step, 4)}

    token_peers = [beside(0, 0, 0), beside(0, 0, 1), beside(1, 0, 0), beside(1, 0, 1), partner]
    peers = token_peers + [{"x": lax.rem(x + 2, 4)}] + [next_row(1, step) for step in (1, -1)]
    if n_z > 1:
        peers += [{"z": lax.rem(z + 1, n_z)}, {"z": lax.rem(z + n_z - 1, n_z)}]
    barrier = pltpu.get_barrier_semaphore()
    for peer in peers:
        pl.semaphore_signal(barrier, inc=1, device_id=peer, device_id_type=MESH_ID)

    sources = (gate_ref, up_ref, down_ref)
    targets = (w_v, next_ref)

    def landing(layer, m):
        return targets[layer].at[:, m, z, 0 if layer else y, x]

    def pre_local(layer, m):
        return pltpu.make_async_copy(
            sources[m].at[layer, pl.ds(owners[layer] * n_exp, n_exp)], landing(layer, m),
            pre_own.at[layer * 3 + m])

    def pre_copy(layer, m, k):
        idx = (layer * 3 + m) * 3 + k - 1
        return remote(sources[m].at[layer, pl.ds(lax.rem(owners[layer] + k, 4) * n_exp, n_exp)],
                      landing(layer, m),
                      pre_send.at[idx], pre_recv.at[idx], {"x": lax.rem(x + k, 4)})

    def hops(along_z):
        return 3 if (n_z if along_z else n_y) > 1 else 0

    def ring_copy(r, m, p):
        step = 1 if p % 2 == 0 else -1
        along_z = (r < 3) == (p < 2)
        if r % 3 >= hops(along_z):
            return None
        pos = z if along_z else y
        i = lax.rem(pos + 4 - step * (r % 3), 4)
        if r < 3:
            piece = w_v.at[p, m, i, y] if along_z else w_v.at[p, m, z, i]
        else:
            piece = w_v.at[p, m, i] if along_z else w_v.at[p, m, :, i]
        idx = (r * 3 + m) * 4 + p
        peer = {"z": lax.rem(z + 4 + step, 4)} if along_z else next_row(0, step)
        return remote(piece, piece, wr_send.at[idx], wr_recv.at[idx], peer)

    def late_copy(stage, hop, p):
        if stage == "rows":
            step = 1 - hop % 2 * 2
            near, far = -step % 4, 2
            if hop < 2:
                src, dst = next_ref.at[p, :, z, 0], next_ref.at[p, :, z, near]
            else:
                xs = pl.ds(n_x // 2 * (hop - 2), n_x // 2)
                src, dst = next_ref.at[p, :, z, near, xs], next_ref.at[p, :, z, far, xs]
            peer = next_row(1, step)
        else:
            if hop >= hops(True):
                return None
            step = 1 - p % 2 * 2
            i = lax.rem(z + 4 - step * hop, 4)
            src = dst = next_ref.at[p, :, i, 0 if stage == "own" else pl.ds(1, n_y - 1)]
            peer = {"z": lax.rem(z + 4 + step, 4)}
        idx = 72 + ({"own": 0, "rows": 3, "rest": 7}[stage] + hop) * 4 + p
        return remote(src, dst, wr_send.at[idx], wr_recv.at[idx], peer)

    def pre_start(layer):
        for m in range(3):
            for k in (1, 3, 2):
                pre_copy(layer, m, k).start()
            pre_local(layer, m).start()

    def pre_wait(layer, m):
        pre_local(layer, m).wait()
        for k in (1, 3, 2):
            pre_copy(layer, m, k).wait_recv()

    def then(before, after):
        if before is not None:
            before.wait_recv()
        if after is not None:
            after.start()

    def ring_event(r, m):
        with jax.named_scope(f"w0r{r}m{m}"):
            if r == 0:
                pre_wait(0, m)
            for p in range(4):
                last = [q for q in range(r) if ring_copy(q, m, p) is not None][-1:]
                after = ring_copy(r, m, p) if r < 6 else None
                if after is not None or r == 6:
                    then(ring_copy(last[0], m, p) if last else None, after)

    def ring_round(r):
        for m in range(3):
            ring_event(r, m)

    def late_event(stage, hop, pair):
        with jax.named_scope(f"w1{stage}{hop}p{pair}"):
            for p in (2 * pair, 2 * pair + 1):
                before = []
                after = [late_copy(stage, hop, p)]
                if stage == "rows":
                    before = [late_copy(stage, q, p) for q in range(2 * hop)]
                    after = [late_copy(stage, 2 * hop + q, p) for q in range(2)]
                elif hop > 0:
                    before = [late_copy(stage, hop - 1, p)]
                elif stage == "rest":
                    before = [late_copy("rows", q, p) for q in (2, 3)]
                for copy in before:
                    then(copy, None)
                for copy in after:
                    then(None, copy)

    def late_end(pair):
        with jax.named_scope(f"w1end{pair}"):
            for p in (2 * pair, 2 * pair + 1):
                then(late_copy("own", 2, p), None)
                then(late_copy("rest", 2, p), None)

    loads = [pltpu.make_async_copy(next_ref.at[e], w_v.at[e], w_sem.at[e]) for e in range(n_exp)]

    def prepare(layer, stream_ref, axis):
        experts = router_ref.shape[1]
        for t in range(2):
            rows = pl.ds((2 * axis + t) * part, part)
            wide = stream_ref[rows, :].astype(jnp.float32)
            inv_rms = lax.rsqrt(jnp.mean(wide * wide, axis=-1, keepdims=True) + NORM_EPS)
            hidden = (wide * inv_rms * norm_ref[layer:layer + 1, :]).astype(jnp.bfloat16)
            h_all[axis, t, 0] = hidden
            logits = lax.dot_general(router_ref[layer], hidden, (((1,), (1,)), ((), ())),
                                     preferred_element_type=jnp.float32)
            ids = lax.broadcasted_iota(jnp.int32, (experts, part), 0)
            chosen = ids < 0
            for j in range(routes_ref.shape[1]):
                chosen |= routes_ref[layer, j:j + 1, (2 * axis + t) * part:(2 * axis + t + 1) * part] == ids
            top = jnp.max(jnp.where(chosen, logits, -jnp.inf), axis=0, keepdims=True)
            weight = jnp.where(chosen, jnp.exp(jnp.where(chosen, logits - top, 0.0)), 0.0)
            gates = weight / jnp.sum(weight, axis=0, keepdims=True)
            g_all[axis, t, 0] = jnp.where(chosen, gates, -1.0)

    def start(copies):
        for copy in copies:
            copy.start()

    def wait_recv(copies):
        for copy in copies:
            copy.wait_recv()

    def wait_send(copies):
        for copy in copies:
            copy.wait_send()

    def early_sends():
        for m in range(3):
            for k in (1, 2, 3):
                pre_copy(0, m, k).wait_send()
            for p in range(4):
                wait_send([copy for copy in (ring_copy(r, m, p) for r in range(6)) if copy is not None])

    def late_sends(last):
        for p in range(4):
            copies = [late_copy("rest", 2, p)]
            if not last:
                copies = [late_copy(stage, hop, p) for stage in ("own", "rest") for hop in range(3)][:5]
                copies += [late_copy("rows", hop, p) for hop in range(4)]
            wait_send([copy for copy in copies if copy is not None])
        if not last:
            for m in range(3):
                for k in (1, 2, 3):
                    pre_copy(1, m, k).wait_send()

    def by_rows(update):
        chunk = min(32, part)

        def body(i, carry):
            update(pl.ds(pl.multiple_of(i * chunk, chunk), chunk), i * chunk, chunk)
            return carry

        lax.fori_loop(0, part // chunk, body, 0)

    def run_layer(layer, stream_ref, halfway=None):
        first = layer == 0
        group = ep * 4 + owners[layer]

        def pair_copy(unit):
            return (
                remote(h_all.at[unit, :, 0], h_all.at[unit, :, 1],
                       agp_send.at[unit], agp_recv.at[unit], partner),
                remote(g_all.at[unit, :, 0], g_all.at[unit, :, 1],
                       agp_send.at[8 + unit], agp_recv.at[8 + unit], partner),
            )

        def gather(axis, kind, t):
            src_kind, src_t, to = {
                (NEAR, 1): (OWN, 0, 0), (MORE, 1): (OWN, 1, 0), (FAR, 0): (NEAR, 1, 0),
                (NEAR, 0): (OWN, 1, 1), (MORE, 0): (OWN, 0, 1), (FAR, 1): (NEAR, 0, 1),
            }[kind, t]
            src, dst = 2 * src_kind + axis, 2 * kind + axis
            idx = 2 * (dst - 2) + t
            peer = beside(layer, axis, to)
            return (
                remote(h_all.at[src, src_t, 0], h_all.at[dst, t, 0],
                       ag_send.at[idx], ag_recv.at[idx], peer),
                remote(g_all.at[src, src_t, 0], g_all.at[dst, t, 0],
                       ag_send.at[12 + idx], ag_recv.at[12 + idx], peer),
            )

        def gather_start(axis):
            for t in range(2):
                start(gather(axis, NEAR, t))
            start(pair_copy(axis))
            for t in range(2):
                start(gather(axis, MORE, t))

        def arrive(kind, axis):
            with jax.named_scope(f"arr{kind}{axis}"):
                for t in range(2):
                    wait_recv(gather(axis, kind, t))
                    if kind == NEAR:
                        start(gather(axis, FAR, 1 - t))
                start(pair_copy(2 * kind + axis))

        def reduce_pair(unit):
            return remote(acc.at[unit, :, 1], pair_in.at[unit],
                          pair_send.at[unit], pair_recv.at[unit], partner)

        def place(unit, t):
            return 2 * (unit - 2) + t + 4 * layer * (unit // 6)

        def reduce_ring(unit, t):
            slot = 2 * (unit - 2) + t
            return remote(acc.at[unit, t, 0], ring_in.at[place(unit, t)], ring_send.at[layer, slot], ring_recv.at[layer, slot],
                          beside(layer, unit % 2, t))

        def add_pair(unit):
            with jax.named_scope("pairw"):
                reduce_pair(unit).wait_recv()

            def update(rows, first_row, n):
                for t in range(2):
                    acc[unit, t, 0, rows] += pair_in[unit, t, rows]

            by_rows(update)

        def add_more(unit):
            with jax.named_scope("morew"):
                reduce_pair(unit).wait_recv()
                far = unit - 2 * (MORE - FAR)
                for t in range(2):
                    reduce_ring(far, t).wait_recv()

            def update(rows, first_row, n):
                for t in range(2):
                    acc[unit, t, 0, rows] += pair_in[unit, t, rows] + ring_in[place(far, t), rows]

            by_rows(update)

        def ring_start(unit):
            for t in range(2):
                reduce_ring(unit, t).start()

        plan = {}

        def at(t, action, *args):
            plan.setdefault(t, []).append((action, args))

        if first:
            for axis in range(2):
                prepare(layer, stream_ref, axis)
            for kind in (NEAR, MORE):
                for axis in range(2):
                    for t in range(2):
                        start(gather(axis, kind, t))
                    if kind == NEAR:
                        start(pair_copy(axis))
        else:
            prepare(layer, stream_ref, 0)
            with jax.named_scope("ready"):
                pl.semaphore_wait(ready, len(token_peers))
            gather_start(0)
        if first:
            for r in range(3):
                ring_round(r)
            arrive(NEAR, 0)
            arrive(NEAR, 1)
            pre_start(1)
            ring_round(3)
            ring_round(4)
            arrive(MORE, 0)
            arrive(MORE, 1)
            ring_round(5)
            arrive(FAR, 0)
            arrive(FAR, 1)
            ring_event(6, 0)
            ring_event(6, 1)
            for m in range(3):
                pre_wait(1, m)
            for pair in range(2):
                late_event("own", 0, pair)
            ring_event(6, 2)
            for pair in range(2):
                late_event("rows", 0, pair)
            for unit in range(UNITS):
                wait_recv(pair_copy(unit))
            for stage, hop, when in LATE_EVENTS:
                for pair in range(2):
                    at(when[pair], late_event, stage, hop, pair)
        else:
            halfway()
            prepare(layer, stream_ref, 1)
            gather_start(1)
            late_end(0)
            start(loads[:2])
            late_sends(last=False)
            arrive(NEAR, 0)
            at(0, loads[0].wait)
            at(1, loads[1].wait)
            at(1, late_end, 1)
            at(1, start, loads[2:])
            at(1, arrive, NEAR, 1)
            at(2, loads[2].wait)
            at(3, loads[3].wait)
            at(3, arrive, MORE, 0)
            at(3, arrive, MORE, 1)
            at(5, arrive, FAR, 0)
            at(7, arrive, FAR, 1)

        def unit_of(k):
            if first:
                return jnp.where(k < 2, k + 2 * FAR, jnp.where(k < 4, k, jnp.where(k < 6, k + 2, k - 6)))
            return jnp.where(k < 6, k + 2, k - 6)

        def step_fn(step, carry):
            k, e = step // n_exp, step % n_exp
            before, late = unit_of(k - 1), unit_of(k - 2)
            kind, late_kind = before // 2, late // 2

            def planned(e_static):
                for t in sorted(plan):
                    if t < steps and t % n_exp == e_static:
                        @pl.when(k == t // n_exp)
                        def _():
                            for action, args in plan[t]:
                                action(*args)

            @pl.when(e == 0)
            def _():
                planned(0)

                @pl.when(k >= 1)
                def _():
                    reduce_pair(before).start()

                if not first:
                    wait_recv(pair_copy(unit_of(k)))

            def sums(mask):
                @pl.when(mask & (k >= 1) & (kind != MORE))
                def _():
                    add_pair(before)

                @pl.when(mask & ((k >= 2) & (late_kind == MORE) if first else (k >= 1) & (kind == MORE)))
                def _():
                    add_more(late if first else before)

            def leave(mask):
                @pl.when(mask & (k >= 1) & (kind != OWN) & ((kind != MORE) if first else True))
                def _():
                    ring_start(before)

                if first:
                    @pl.when(mask & (k >= 2) & (late_kind == MORE))
                    def _():
                        ring_start(late)

            hurry = k == 1 if first else (k == 4) | (k == 6)

            @pl.when(e == 1)
            def _():
                planned(1)
                sums(hurry)

            @pl.when(e == 2)
            def _():
                planned(2)
                sums(jnp.logical_not(hurry))
                leave(hurry)

            @pl.when(e == 3)
            def _():
                planned(3)
                leave(jnp.logical_not(hurry))

            unit = unit_of(k)
            with jax.named_scope("load"):
                tokens = h_all[unit].reshape(-1, d_model)
            gate_w = w_v[e, 0].reshape(-1, d_model)
            up_w = w_v[e, 1].reshape(-1, d_model)
            down_w = w_v[e, 2].reshape(-1, d_model)
            d_ff = gate_w.shape[0]
            inner = []
            for f in range(0, d_ff, 256):
                nt = (((1,), (1,)), ((), ()))
                u = lax.dot_general(tokens, gate_w[f:f + 256], nt, preferred_element_type=jnp.float32)
                v = lax.dot_general(tokens, up_w[f:f + 256], nt, preferred_element_type=jnp.float32)
                inner.append((jax.nn.silu(u) * v).astype(jnp.bfloat16))
            inner = jnp.concatenate(inner, axis=1)
            row = group * n_exp + e
            gate_cols = []
            for t in range(2):
                for s in range(2):
                    gates = g_all[unit, t, s, pl.ds(row, 1), :]
                    gate_cols.append(jnp.broadcast_to(gates, (128, part)).T)
            gate_b = jnp.concatenate(gate_cols, axis=0)
            gate_b = jnp.concatenate([gate_b, gate_b], axis=1)
            start_sum = e == 0
            for c in range(0, d_model, 256):
                o = jnp.dot(inner, down_w[:, c:c + 256], preferred_element_type=jnp.float32)
                o = o.astype(jnp.bfloat16).astype(jnp.float32)
                new = jnp.where(gate_b >= 0.0, gate_b * o, 0.0).reshape(2, 2, part, 256)
                prev = jnp.where(start_sum, 0.0, acc[unit, :, :, :, c:c + 256])
                acc[unit, :, :, :, c:c + 256] = prev + new
            return carry

        lax.fori_loop(0, steps, step_fn, 0)
        reduce_pair(1).start()
        for t in sorted(plan):
            if t >= steps:
                for action, args in plan[t]:
                    action(*args)

        def end_near(axis):
            near = 2 * NEAR + axis
            for t in range(2):
                with jax.named_scope("fin1"):
                    reduce_ring(near, 1 - t).wait_recv()

                def update(rows, first_row, n):
                    own = pl.ds(pl.multiple_of((2 * axis + t) * part + first_row, n), n)
                    acc[axis, t, 0, rows] += stream_ref[own, :].astype(jnp.float32) + ring_in[place(near, 1 - t), rows]

                by_rows(update)

        def end_more(axis):
            more = 2 * MORE + axis
            for t in range(2):
                with jax.named_scope("fin2"):
                    reduce_ring(more, t).wait_recv()

                def update(rows, first_row, n):
                    own = pl.ds(pl.multiple_of((2 * axis + t) * part + first_row, n), n)
                    out_ref[own, :] = (acc[axis, t, 0, rows] + ring_in[place(more, t), rows]).astype(out_ref.dtype)

                by_rows(update)

        def end_sends():
            for axis in range(2):
                for t in range(2):
                    reduce_ring(2 * MORE + axis, t).wait_send()

        end_near(0)
        if not first:
            end_more(0)
        add_pair(1)
        end_near(1)
        for unit in range(UNITS):
            wait_send(pair_copy(unit))
            reduce_pair(unit).wait_send()
            if unit >= 2:
                for t in range(2):
                    wait_send(gather(unit % 2, unit // 2, t))
                    if unit < 2 * MORE:
                        reduce_ring(unit, t).wait_send()
        return end_more, end_sends

    with jax.named_scope("barrier"):
        pl.semaphore_wait(barrier, len(peers))
    pre_start(0)
    end_more, end_sends = run_layer(0, x_ref)
    early_sends()
    for peer in token_peers:
        pl.semaphore_signal(ready, inc=1, device_id=peer, device_id_type=MESH_ID)
    end_more(0)

    def halfway():
        end_more(1)
        end_sends()

    end_more_1, end_sends_1 = run_layer(1, out_ref, halfway)
    end_more_1(1)
    end_sends_1()
    late_sends(last=True)


def moe_layers(ring_shape, stream, norm_w, router, routes, weights):
    tok_dev, d_model = stream.shape
    part = tok_dev // 4
    n_z, n_y, n_x = ring_shape
    vmem = pl.BlockSpec(memory_space=pltpu.VMEM)
    hbm = pl.BlockSpec(memory_space=pl.ANY)
    dma = pltpu.SemaphoreType.DMA
    n_exp, f_dev = weights[0].shape[1] // n_x, weights[0].shape[2]
    w_shape = (n_exp, 3, n_z, n_y, n_x, f_dev, d_model)
    return pl.pallas_call(
        functools.partial(kernel, ring_shape),
        name="moe_layers",
        out_shape=[jax.ShapeDtypeStruct(stream.shape, stream.dtype), jax.ShapeDtypeStruct(w_shape, jnp.bfloat16)],
        in_specs=[vmem] * 4 + [hbm] * 3,
        out_specs=[vmem, hbm],
        scratch_shapes=[
            pltpu.VMEM((UNITS, 2, 2, part, d_model), jnp.bfloat16),
            pltpu.VMEM((UNITS, 2, 2, router.shape[1], part), jnp.float32),
            pltpu.VMEM(w_shape, jnp.bfloat16),
            pltpu.VMEM((UNITS, 2, 2, part, d_model), jnp.float32),
            pltpu.VMEM((UNITS, 2, part, d_model), jnp.float32),
            pltpu.VMEM((16, part, d_model), jnp.float32),
            dma((24,)), dma((24,)), dma((16,)), dma((16,)), dma((8,)), dma((8,)), dma((2, 12)), dma((2, 12)),
            dma((6,)), dma((18,)), dma((18,)), dma((112,)), dma((112,)), dma((n_exp,)),
            pltpu.SemaphoreType.REGULAR,
        ],
        compiler_params=pltpu.CompilerParams(
            collective_id=0, has_side_effects=True, vmem_limit_bytes=67043328),
        cost_estimate=pl.CostEstimate(flops=104 * 10**9, bytes_accessed=64 * 2**20, transcendentals=0),
    )(stream, norm_w, router, routes, *weights)[0]


def solution(mesh):
    n_x = 4
    n_y = min(4, mesh.shape["fsdp"] // n_x)
    devices = mesh.devices.reshape(mesh.shape["rep"], mesh.shape["ep"], -1, n_y, n_x)
    cells = Mesh(devices, ("rep", "ep", "z", "y", "x"))
    ring_shape = devices.shape[2:]
    fsdp = ("z", "y", "x")
    token_spec = P(("rep", "ep") + fsdp, None)
    expert_in_spec = P(None, "ep", None, fsdp)
    expert_out_spec = P(None, "ep", fsdp, None)
    route_spec = P(None, ("rep", "ep") + fsdp, None)

    def device_step(x_in, norm_w, router_w, gate_w, up_w, down_w, routes):
        shards = (gate_w.transpose(0, 1, 3, 2), up_w.transpose(0, 1, 3, 2), down_w)
        return moe_layers(ring_shape, x_in, norm_w, router_w.transpose(0, 2, 1), routes.transpose(0, 2, 1), shards)

    return jax.shard_map(device_step, mesh=cells,
                         in_specs=(token_spec, P(), P(), expert_in_spec, expert_in_spec, expert_out_spec, route_spec),
                         out_specs=token_spec, check_vma=False)
```
